32 devices in a mesh: shard: 4 (over x, core), rep: 8 (over z, y).
Axes of the slice: x: 2, y: 2, z: 4, core: 2. Of those that a mesh axis runs over, the one named last changes fastest.
Arguments:
- tokens: bfloat16 [12288, 4608], P(('shard', 'rep')), may hold values from -6 to 6
- norm_gain: float32 [4608], replicated, may hold values from 0.25 to 1.75
- key_grad: bfloat16 [12288, 1024], P(('shard', 'rep')), may hold values from -6 to 6
- key_weight: bfloat16 [4608, 1024], P('shard'), may hold values from -0.09375 to 0.09375
- m_code: bfloat16 [4608, 1024], P('shard'), may hold values from -127 to 127, as said below
- m_exp: int32 [4608, 4], P('shard'), may hold values from 3 to 7
- v_code: bfloat16 [4608, 1024], P('shard'), may hold values from 1 to 255, as said below
- v_exp: int32 [4608, 4], P('shard'), may hold values from 4 to 9
Outputs:
- keys: bfloat16 [12288, 1024], P(('shard', 'rep'))
- token_grad: bfloat16 [12288, 4608], P(('shard', 'rep'))
- adam_step: float32 [4608, 1024], P('shard')
- m_rel: bfloat16 [4608, 1024], P('shard')
- m_scale: float32 [4608, 4], P('shard')
- v_rel: bfloat16 [4608, 1024], P('shard')
- v_scale: float32 [4608, 4], P('shard')
The draws below stay inside these ranges and needn't reach their ends.
Inputs may be any that keep to these rules, and one draw needn't show every extreme that they name: `m_code`: whole numbers. `v_code`: whole numbers.
All inputs are finite; a program needn't handle non-finite values. Where the reference program divides by a largest or mean magnitude, that divisor is 1e-20 or more.
Results may differ from the reference program's by a relative error of at most 0.0099.
Values may be sent and summed in bfloat16 or wider, within the bound.
A program may use at most 192 MiB of HBM per device.

```python
import jax
import jax.numpy as jnp
from jax import lax

D = 4608
KH = 1024
NB = 4
TOKENS = 12288


def draw_m_code(key, part):
    return jax.random.randint(key, (D, KH), -127, 128).astype(jnp.float32).astype(jnp.bfloat16)


def draw_v_code(key, part):
    return jax.random.randint(key, (D, KH), 1, 256).astype(jnp.float32).astype(jnp.bfloat16)


def place_ends(values, stream_key, smallest, largest):
    extent = values.shape
    index_at = [jax.random.randint(jax.random.fold_in(stream_key, axis), (), 0, extent[axis]) for axis in range(len(extent))]
    values = values.at[tuple(index_at)].set(smallest)
    longest = extent.index(max(extent))
    index_at[longest] = (index_at[longest] + 1) % extent[longest]
    return values.at[tuple(index_at)].set(largest)


def steps_of(own_key, dims, shards, smallest, largest):
    def one(dim, parts):
        steps = jax.random.uniform(jax.random.fold_in(jax.random.fold_in(own_key, 6), dim), (parts,), jnp.float32, smallest / len(shards), largest / len(shards))
        return jnp.repeat(jnp.exp(steps), dims[dim] // parts).reshape((-1,) + (1,) * (len(dims) - dim - 1))

    level = one(*shards[0])
    for cut in shards[1:]:
        level = level * one(*cut)
    return level


def bell_draw(stream_key, dims, scale, most, split=(), kind=jnp.bfloat16):
    drawn = scale * jax.random.normal(stream_key, dims, jnp.float32)
    if split:
        drawn = drawn * steps_of(stream_key, dims, split, -0.22, 0.18)
    return jnp.clip(drawn, -most, most).astype(kind)


def setup_inputs(seed: int = 0) -> dict:
    streams_of = jax.random.split(jax.random.key(seed), 9)
    return {
        "tokens": bell_draw(streams_of[0], (TOKENS, D), 1.0, 6.0, ((0, 32),)),
        "norm_gain": jnp.clip(1.0 + 0.15 * jax.random.normal(streams_of[1], (D,), jnp.float32), 0.25, 1.75),
        "key_grad": bell_draw(streams_of[2], (TOKENS, KH), 1.0, 6.0, ((0, 32),)),
        "key_weight": bell_draw(streams_of[3], (D, KH), D ** -0.5, 0.09375, ((0, 4),)),
        "m_code": draw_m_code(jax.random.fold_in(streams_of[8], 71), 0),
        "m_exp": place_ends(jax.random.randint(streams_of[5], (D, NB), 3, 8), jax.random.fold_in(streams_of[5], 1), 3, 7).astype(jnp.int32),
        "v_code": draw_v_code(jax.random.fold_in(streams_of[8], 71), 0),
        "v_exp": place_ends(jax.random.randint(streams_of[7], (D, NB), 4, 10), jax.random.fold_in(streams_of[7], 1), 4, 9).astype(jnp.int32),
    }


bias_first = 0.9999734386011124
bias_second = 0.0952078528862904

def requantize(grad, m_code, m_exp, v_code, v_exp):
    rows, width = grad.shape
    blocks = m_exp.shape[1]
    size = width // blocks
    g3 = grad.reshape(rows, blocks, size)
    m_old = m_code.astype(jnp.float32).reshape(rows, blocks, size) * (jnp.exp2(m_exp.astype(jnp.float32)) / 127.0)[:, :, None]
    v_old = v_code.astype(jnp.float32).reshape(rows, blocks, size) * (jnp.exp2(v_exp.astype(jnp.float32)) / 255.0)[:, :, None]
    m_new = 0.9 * m_old + 0.1 * g3
    v_new = 0.999 * v_old + 0.001 * g3 * g3
    step = m_new / bias_first / (jnp.sqrt(v_new / bias_second) + 1e-08)
    m_scale = lax.optimization_barrier(jnp.max(jnp.abs(m_new), axis=2))
    v_scale = lax.optimization_barrier(jnp.max(v_new, axis=2))
    m_rel = (m_new / (m_scale + 1e-06)[:, :, None]).reshape(rows, width).astype(jnp.bfloat16)
    v_rel = (v_new / (v_scale + 1e-06)[:, :, None]).reshape(rows, width).astype(jnp.bfloat16)
    return (step.reshape(rows, width), m_rel, m_scale, v_rel, v_scale)

def reference(tokens, norm_gain, key_grad, key_weight, m_code, m_exp, v_code, v_exp):
    x = tokens.astype(jnp.float32)
    inv = lax.rsqrt(lax.optimization_barrier(jnp.mean(x * x, axis=1, keepdims=True)) + 1e-06)
    normed = (x * inv * norm_gain).astype(jnp.bfloat16)
    keys = jnp.dot(normed, key_weight, preferred_element_type=jnp.float32).astype(jnp.bfloat16)
    dnormed = lax.dot_general(key_grad, key_weight, (((1,), (1,)), ((), ())), preferred_element_type=jnp.float32)
    scaled = dnormed * norm_gain
    inner = lax.optimization_barrier(jnp.mean(scaled * x, axis=1, keepdims=True))
    token_grad = (inv * scaled - x * inv * inv * inv * inner).astype(jnp.bfloat16)
    grad = lax.dot_general(normed, key_grad, (((0,), (0,)), ((), ())), preferred_element_type=jnp.float32)
    step, m_rel, m_scale, v_rel, v_scale = requantize(grad, m_code, m_exp, v_code, v_exp)
    return (keys, token_grad, step, m_rel, m_scale, v_rel, v_scale)
```

```python
import functools

import jax
import jax.numpy as jnp
from jax import lax
from jax.experimental import pallas as pl
from jax.experimental.pallas import tpu as pltpu
from jax.sharding import PartitionSpec as P

bias_first = 0.9999734386011124
bias_second = 0.0952078528862904
F32 = jnp.float32
BF16 = jnp.bfloat16

HALVES = [("x", "y", "l"), ("y", "l", "x"), ("l", "x", "y"), ("x", "y", "l")]
DOUBLES = [("l", "y"), ("y", "l"), ("l", "y"), ("y", "l")]
HELPERS = ["y", "l", "y", "l"]
ORDER = [
    "WX0", "WX1", "NORM", "T0", "T1", "O0", "T2", "O1", "T3", "WF0", "WF1", "WC", "O2", "O3",
    "C20", "C21", "WG0", "WG1", "C22", "MO", "C30", "C31", "C23", "C32", "MC", "WX2", "WX3",
    "C40", "C41", "C42", "C33", "C50", "C51", "C52", "C43", "C60", "C61", "C62", "WF2", "WF3", "C53",
    "C70", "C71", "C72", "WG2", "WG3", "MF", "C63", "MG", "FIN", "C73",
]


def bits_of(count):
    bits = count.bit_length() - 1
    assert 1 << bits == count
    return bits


class Labels:
    def __init__(self, counts):
        shards, reps = bits_of(counts["shard"]), bits_of(counts["rep"])
        assert shards == 2 and reps >= 2
        self.me = {axis: lax.axis_index(axis) for axis in ("shard", "rep")}
        self.of = {"c": ("shard", 0), "x": ("shard", 1), "y": ("rep", 0), "l": ("rep", 1)}
        self.extra = [f"h{n}" for n in range(2, reps)]
        for n in range(2, reps):
            self.of[f"h{n}"] = ("rep", n)
        self.bit = {}
        for label, (axis, n) in self.of.items():
            self.bit[label] = lax.rem(lax.div(self.me[axis], jnp.int32(1 << n)), jnp.int32(2))

    def device(self, label):
        axis, n = self.of[label]
        return {axis: self.me[axis] + (1 << n) - 2 * (1 << n) * self.bit[label]}


def tiled(rows, step, body):
    def run(i, carry):
        body(pl.ds(pl.multiple_of(i * step, step), step))
        return carry

    lax.fori_loop(0, rows // step, run, 0)


def step_of(rows, most):
    for step in range(most, 0, -1):
        if rows % step == 0 and step % 16 == 0:
            return step
    return rows


def layer_kernel(counts, tokens, gain, key_grad, weight, keys, token_grad, grads, *scratch):
    (x, gains, kg, normed, turned, full, own, th, kc, s1, r1, s2, r2, s3, r3, hs, hr, got, kacc, dn, tg, kout, invs,
     load_sem, out_sem, core_sem, one_sem, two_sem, three_sem, h_sem, a_sem, w_sem, wc_sem, wo_sem) = scratch
    lab = Labels(counts)
    bit = lab.bit
    tokens_here, features = x.shape
    groups, _, _, part, wide = own.shape
    rows = 4 * part
    width = kg.shape[1]
    shard = lab.me["shard"]
    core = bit["c"]
    unit = rows // (2 * len(HELPERS))

    def local(src, dst, sem):
        return pltpu.make_async_copy(src, dst, sem)

    def remote(src, dst, sems, label):
        return pltpu.make_async_remote_copy(
            src_ref=src, dst_ref=dst, send_sem=sems.at[0], recv_sem=sems.at[1],
            device_id=lab.device(label), device_id_type=pl.DeviceIdType.MESH,
        )

    sent = []

    def send(copy):
        copy.start()
        sent.append(copy)
        return copy

    third = tokens_here // 3
    loads = [local(tokens.at[pl.ds(n * third, third)], x.at[pl.ds(n * third, third)], load_sem.at[n]) for n in range(3)]
    load_gain = local(gain, gains, load_sem.at[3])
    load_kg = local(key_grad, kg, load_sem.at[4])
    load_w = local(weight, full.at[shard], load_sem.at[5])
    load_gain.start()
    for load in loads:
        load.start()
    load_kg.start()
    load_w.start()

    barrier = pltpu.get_barrier_semaphore()
    for label in lab.of:
        pl.semaphore_signal(barrier, inc=1, device_id=lab.device(label), device_id_type=pl.DeviceIdType.MESH)
    pl.semaphore_wait(barrier, len(lab.of))

    far = shard + 2 - 4 * bit["x"]
    near = shard + 1 - 2 * core
    both = far + 1 - 2 * core

    def rows_at(place):
        return (2 * place["x"] + place["c"]) * rows + (2 * place["y"] + place["l"]) * part

    tasks = {}

    def unit_at(n, side):
        return pl.ds(pl.multiple_of((2 * n + side) * unit, 16 if unit % 16 == 0 else unit), unit)

    def weight_copies(n):
        side = bit[HELPERS[n]]
        mine, other = unit_at(n, side), unit_at(n, 1 - side)
        return dict(
            wx=remote(weight.at[mine], full.at[shard, mine], w_sem.at[n, 0], "x"),
            wf=remote(full.at[far, mine], full.at[far, mine], w_sem.at[n, 1], HELPERS[n]),
            wc=remote(full.at[far, mine], full.at[far, mine], wc_sem.at[n, 0], "c"),
            wd=remote(full.at[far, other], full.at[far, other], wc_sem.at[n, 1], "c"),
        )

    parts = [weight_copies(n) for n in range(len(HELPERS))]

    def weight_task(n):
        def wx():
            send(parts[n]["wx"])

        def wf():
            parts[n]["wx"].wait_recv()
            send(parts[n]["wf"])
            send(parts[n]["wc"])

        def wg():
            parts[n]["wf"].wait_recv()
            send(parts[n]["wd"])

        tasks[f"WX{n}"], tasks[f"WF{n}"], tasks[f"WG{n}"] = wx, wf, wg

    for n in range(len(HELPERS)):
        weight_task(n)
    own_copy = remote(full.at[shard], full.at[shard], wo_sem, "c")

    def weight_core():
        load_w.wait()
        send(own_copy)

    tasks["WC"] = weight_core

    def norm():
        load_gain.wait()
        flat = jnp.concatenate([gains[k : k + 1, :] for k in range(features // gains.shape[1])], axis=1)

        def block(at):
            value = x[at, :].astype(F32)
            inv = lax.rsqrt(jnp.mean(value * value, axis=1, keepdims=True) + 1e-06)
            invs[at, :] = inv
            normed[at, :] = (value * inv * flat).astype(BF16)

        for n in range(3):
            loads[n].wait()

            def run(i, carry):
                block(pl.ds(pl.multiple_of(n * third + i * 16, 16), 16))
                return carry

            lax.fori_loop(0, third // 16, run, 0)

        def turn(at):
            turned[at, :] = normed[:, at].T

        tiled(features, 128, turn)
        load_kg.wait()

    tasks["NORM"] = norm

    def outer(place, g):
        at = pl.ds(pl.multiple_of(rows_at(place), 16), part)
        return jnp.dot(turned[at, :], kg[:, g * wide : (g + 1) * wide], preferred_element_type=F32)

    core_copies = [remote(th.at[g], kc.at[g], core_sem.at[g], "c") for g in range(groups)]

    def group_tasks(g):
        o1, o2, o3 = HALVES[g]
        a1, a2 = DOUBLES[g]
        b1, b2, b3 = bit[o1], bit[o2], bit[o3]

        def theirs():
            def run(t, carry):
                a, b = t // 4, t % 4
                place = {"x": a, "c": 1 - core, "y": b // 2, "l": b % 2}
                th[g, a, b] = outer(place, g).astype(BF16)
                return carry

            lax.fori_loop(0, 8, run, 0)
            send(core_copies[g])

        one = [remote(s1.at[g, j], r1.at[g, j], one_sem.at[g, n], o1) for n, j in enumerate((1 - b2, b2))]
        two = [remote(s2.at[g, j], r2.at[g, j], two_sem.at[g, n], o2) for n, j in enumerate((1 - b3, b3))]
        three = remote(s3.at[g], r3.at[g], three_sem.at[g], o3)
        more = [remote(hs.at[g, n], hr.at[g, n], h_sem.at[g, n], label) for n, label in enumerate(lab.extra)]
        spot = {"y": bit["y"], "l": bit["l"]}
        mine = got.at[g, spot["y"], spot["l"]]
        across = dict(spot)
        across[a1] = 1 - spot[a1]
        other = got.at[g, across["y"], across["l"]]
        up1 = remote(mine, mine, a_sem.at[g, 0], a1)
        up2 = remote(mine, mine, a_sem.at[g, 1], a2)
        up3 = remote(other, other, a_sem.at[g, 2], a2)

        def ours():
            core_copies[g].wait_recv()

            def piece(first, second, third_bit):
                place = {o1: first, o2: second, o3: third_bit, "c": core}
                came = kc[g, place["x"], 2 * place["y"] + place["l"]]
                return outer(place, g) + came.astype(F32)

            for n, j in enumerate((1 - b2, b2)):
                def run(t, carry):
                    s1[g, j, t] = piece(1 - b1, j, t).astype(BF16)
                    return carry

                lax.fori_loop(0, 2, run, 0)
                send(one[n])

            def keep(t, carry):
                own[g, t // 2, t % 2] = piece(b1, t // 2, t % 2)
                return carry

            lax.fori_loop(0, 4, keep, 0)

        step = step_of(part, 96)

        def second():
            one[0].wait_recv()
            for n, j in enumerate((1 - b3, b3)):
                def add(at):
                    s2[g, j, at, :] = (own[g, 1 - b2, j, at, :] + r1[g, 1 - b2, j, at, :].astype(F32)).astype(BF16)

                tiled(part, step, add)
                send(two[n])

        def third_step():
            one[1].wait_recv()
            two[0].wait_recv()

            def add(at):
                total = own[g, b2, 1 - b3, at, :] + r1[g, b2, 1 - b3, at, :].astype(F32)
                s3[g, at, :] = (total + r2[g, 1 - b3, at, :].astype(F32)).astype(BF16)

            tiled(part, step, add)
            send(three)

        def fourth():
            two[1].wait_recv()
            three.wait_recv()

            def add(at):
                total = own[g, b2, b3, at, :] + r1[g, b2, b3, at, :].astype(F32)
                total = total + r2[g, b3, at, :].astype(F32) + r3[g, at, :].astype(F32)
                if more:
                    hs[g, 0, at, :] = total.astype(BF16)
                else:
                    got[g, bit["y"], bit["l"], at, :] = total.astype(BF16)

            tiled(part, step, add)
            if more:
                send(more[0])

        def fifth():
            for n in range(len(more)):
                more[n].wait_recv()
                last = n + 1 == len(more)

                def add(at):
                    total = (hs[g, n, at, :].astype(F32) + hr[g, n, at, :].astype(F32)).astype(BF16)
                    if last:
                        got[g, bit["y"], bit["l"], at, :] = total
                    else:
                        hs[g, n + 1, at, :] = total

                tiled(part, step, add)
                if not last:
                    send(more[n + 1])
            send(up1)
            send(up2)

        def sixth():
            up1.wait_recv()
            send(up3)

        def seventh():
            up2.wait_recv()
            up3.wait_recv()
            for a in range(2):
                for b in range(2):
                    out = grads.at[2 * a + b, :, pl.ds(g * wide, wide)]
                    put(local(got.at[g, a, b], out, out_sem.at[g, 2 * a + b]))

        names = dict(T=theirs, O=ours, C2=second, C3=third_step, C4=fourth, C5=fifth, C6=sixth, C7=seventh)
        for name, task in names.items():
            tasks[f"{name}{g}"] = task

    written = []

    def put(copy):
        copy.start()
        written.append(copy)

    for g in range(groups):
        group_tasks(g)

    def matmuls(index, first):
        base = pl.multiple_of(index * rows, 128)

        def key_part(t, carry):
            at = pl.ds(pl.multiple_of(t * 256, 256), 256)
            total = jnp.dot(normed[:, pl.ds(base, rows)], full[index, :, at], preferred_element_type=F32)
            if first:
                kacc[:, at] = total
            else:
                kacc[:, at] += total
            return carry

        lax.fori_loop(0, width // 256, key_part, 0)
        cut = 384

        def back_part(t, carry):
            at = pl.ds(pl.multiple_of(t * cut, 128), cut)
            to = pl.ds(pl.multiple_of(base + t * cut, 128), cut)
            dn[:, to] = lax.dot_general(
                kg[...], full[index, at, :], (((1,), (1,)), ((), ())), preferred_element_type=F32
            )
            return carry

        lax.fori_loop(0, rows // cut, back_part, 0)

    def mo():
        matmuls(shard, True)

    def mc():
        own_copy.wait_recv()
        matmuls(near, False)

    def mf():
        matmuls(far, False)

    def mg():
        for n in range(len(HELPERS)):
            parts[n]["wc"].wait_recv()
            parts[n]["wd"].wait_recv()
        matmuls(both, False)

    tasks.update(MO=mo, MC=mc, MF=mf, MG=mg)

    def finish():
        flat = jnp.concatenate([gains[k : k + 1, :] for k in range(features // gains.shape[1])], axis=1)
        for n in range(3):
            def run(i, carry):
                at = pl.ds(pl.multiple_of(n * third + i * 16, 16), 16)
                kout[at, :] = kacc[at, :].astype(BF16)
                value = x[at, :].astype(F32)
                inv = invs[at, :]
                scaled = dn[at, :] * flat
                inner = jnp.mean(scaled * value, axis=1, keepdims=True)
                tg[at, :] = (inv * scaled - value * (inv * inv * inv * inner)).astype(BF16)
                return carry

            lax.fori_loop(0, third // 16, run, 0)
            at = pl.ds(n * third, third)
            put(local(tg.at[at], token_grad.at[at], out_sem.at[groups, n]))
        put(local(kout, keys, out_sem.at[groups, 3]))

    tasks["FIN"] = finish

    assert sorted(ORDER) == sorted(tasks)
    for name in ORDER:
        tasks[name]()
    for copy in written:
        copy.wait()
    for copy in sent:
        copy.wait_send()


def layer(counts, tokens, gain, key_grad, weight):
    count, features = tokens.shape
    width = key_grad.shape[1]
    rows = weight.shape[0]
    groups = len(HALVES)
    wide = width // groups
    part = rows // 4
    extra = max(bits_of(counts["rep"]) - 2, 1)
    lanes = 128
    any_space = pl.BlockSpec(memory_space=pl.ANY)
    dma = pltpu.SemaphoreType.DMA
    helpers = len(HELPERS)
    scratch = [
        pltpu.VMEM((count, features), BF16),
        pltpu.VMEM((features // lanes, lanes), F32),
        pltpu.VMEM((count, width), BF16),
        pltpu.VMEM((count, features), BF16),
        pltpu.VMEM((features, count), BF16),
        pltpu.VMEM((4, rows, width), BF16),
        pltpu.VMEM((groups, 2, 2, part, wide), F32),
        pltpu.VMEM((groups, 2, 4, part, wide), BF16),
        pltpu.VMEM((groups, 2, 4, part, wide), BF16),
        pltpu.VMEM((groups, 2, 2, part, wide), BF16),
        pltpu.VMEM((groups, 2, 2, part, wide), BF16),
        pltpu.VMEM((groups, 2, part, wide), BF16),
        pltpu.VMEM((groups, 2, part, wide), BF16),
        pltpu.VMEM((groups, part, wide), BF16),
        pltpu.VMEM((groups, part, wide), BF16),
        pltpu.VMEM((groups, extra, part, wide), BF16),
        pltpu.VMEM((groups, extra, part, wide), BF16),
        pltpu.VMEM((groups, 2, 2, part, wide), BF16),
        pltpu.VMEM((count, width), F32),
        pltpu.VMEM((count, features), F32),
        pltpu.VMEM((count, features), BF16),
        pltpu.VMEM((count, width), BF16),
        pltpu.VMEM((count, 1), F32),
        dma((6,)),
        dma((groups + 1, 4)),
        dma((groups, 2)),
        dma((groups, 2, 2)),
        dma((groups, 2, 2)),
        dma((groups, 2)),
        dma((groups, extra, 2)),
        dma((groups, 3, 2)),
        dma((helpers, 2, 2)),
        dma((helpers, 2, 2)),
        dma((2,)),
    ]
    keys, token_grad, grads = pl.pallas_call(
        functools.partial(layer_kernel, counts),
        in_specs=[any_space] * 4,
        out_specs=[any_space] * 3,
        out_shape=[
            jax.ShapeDtypeStruct((count, width), BF16),
            jax.ShapeDtypeStruct((count, features), BF16),
            jax.ShapeDtypeStruct((4, part, width), BF16),
        ],
        scratch_shapes=scratch,
        compiler_params=pltpu.CompilerParams(
            collective_id=0, has_side_effects=True, vmem_limit_bytes=67043328
        ),
        name="layer",
    )(tokens, gain.reshape(features // lanes, lanes), key_grad, weight)
    return keys, token_grad, grads.reshape(rows, width)


def requantize_kernel(chunks, grads, m_code, m_exp, v_code, v_exp, step, m_rel, m_scale, v_rel, v_scale):
    size = m_code.shape[1] // chunks
    units = jnp.concatenate(
        [jnp.exp2(m_exp[...].astype(F32)) / 127.0, jnp.exp2(v_exp[...].astype(F32)) / 255.0], axis=0
    ).T
    tops = []
    for c in range(chunks):
        cols = slice(c * size, (c + 1) * size)
        g = grads[:, cols].astype(F32)
        m_old = m_code[:, cols].astype(F32) * units[:, c : c + 1]
        v_old = v_code[:, cols].astype(F32) * units[:, chunks + c : chunks + c + 1]
        m_new = 0.9 * m_old + 0.1 * g
        v_new = 0.999 * v_old + 0.001 * g * g
        step[:, cols] = (m_new * (1.0 / bias_first)) / (jnp.sqrt(v_new * (1.0 / bias_second)) + 1e-08)
        m_top = jnp.max(jnp.abs(m_new), axis=1, keepdims=True)
        v_top = jnp.max(v_new, axis=1, keepdims=True)
        tops.append((m_top, v_top))
        m_rel[:, cols] = (m_new * (1.0 / (m_top + 1e-06))).astype(BF16)
        v_rel[:, cols] = (v_new * (1.0 / (v_top + 1e-06))).astype(BF16)
    turned = jnp.concatenate([m for m, _ in tops] + [v for _, v in tops], axis=1).T
    m_scale[...] = turned[:chunks]
    v_scale[...] = turned[chunks:]


def requantize(grads, m_code, m_exp, v_code, v_exp):
    rows, width = m_code.shape
    chunks = m_exp.shape[1]
    block = 128
    wide = pl.BlockSpec((block, width), lambda i: (i, 0))
    thin = pl.BlockSpec((chunks, block), lambda i: (0, i))
    shape = jax.ShapeDtypeStruct
    step, m_rel, m_scale, v_rel, v_scale = pl.pallas_call(
        functools.partial(requantize_kernel, chunks),
        grid=(rows // block,),
        in_specs=[wide, wide, thin, wide, thin],
        out_specs=[wide, wide, thin, wide, thin],
        out_shape=[
            shape((rows, width), F32),
            shape((rows, width), BF16),
            shape((chunks, rows), F32),
            shape((rows, width), BF16),
            shape((chunks, rows), F32),
        ],
        name="requantize",
    )(grads, m_code, m_exp.T, v_code, v_exp.T)
    return step, m_rel, m_scale.T, v_rel, v_scale.T


def body(counts, tokens, norm_gain, key_grad, key_weight, m_code, m_exp, v_code, v_exp):
    keys, token_grad, grads = layer(counts, tokens, norm_gain, key_grad, key_weight)
    return (keys, token_grad, *requantize(grads, m_code, m_exp, v_code, v_exp))


def solution(mesh):
    rows = P("shard", None)
    tokens = P(("shard", "rep"), None)
    return jax.shard_map(
        functools.partial(body, dict(mesh.shape)),
        mesh=mesh,
        in_specs=(tokens, P(), tokens, rows, rows, rows, rows, rows),
        out_specs=(tokens, tokens, rows, rows, rows, rows, rows),
        check_vma=False,
    )
```

```python
import functools

import jax
import jax.numpy as jnp
from jax import lax
from jax.experimental import pallas as pl
from jax.experimental.pallas import tpu as pltpu
from jax.sharding import PartitionSpec as P

bias_first = 0.9999734386011124
bias_second = 0.0952078528862904
F32 = jnp.float32
BF16 = jnp.bfloat16

HALVES = [("x", "y"), ("y", "x"), ("x", "y"), ("y", "x")]
SPREADS = [2, 2, 4]
ORDER = [
    "N0", "GATE", "WX0", "WC", "N1", "N2", "WX2", "RT", "KO", "T1", "T0", "RO", "T3", "WF0", "O1", "O0", "C210",
    "KC", "WF2", "C201", "C200", "BC", "WX1", "C301", "QA2", "O3", "QB2", "T2", "BO", "C310", "C300", "QC2",
    "O2", "QE2", "C401", "C410", "C501", "C400", "C211", "WF1", "C220", "QD2", "C230", "WG0", "C221", "C320",
    "C510", "C420", "C321", "E501", "C500", "E510", "WG1", "C421", "C520", "C311", "C231", "C411", "C521", "KG",
    "C330", "E500", "C331", "C430", "E520", "C511", "KF", "C431", "C530", "E521", "C70", "BF", "E511", "C531",
    "BG", "F0", "E530", "F1", "E531", "C71", "C72", "F2", "C73",
]


def bits_of(count):
    bits = count.bit_length() - 1
    assert 1 << bits == count
    return bits


class Labels:
    def __init__(self, counts):
        shards, reps = bits_of(counts["shard"]), bits_of(counts["rep"])
        assert shards == 2 and reps >= 3
        self.me = {axis: lax.axis_index(axis) for axis in ("shard", "rep")}
        self.of = {"c": ("shard", 0), "x": ("shard", 1), "y": ("rep", 0), "l": ("rep", 1)}
        self.extra = [f"h{n}" for n in range(3, reps)]
        for n in range(3, reps):
            self.of[f"h{n}"] = ("rep", n)
        self.bit = {label: self.digit(axis, 1 << n, 2) for label, (axis, n) in self.of.items()}
        self.place = self.digit("rep", 2, 4)
        self.inner = lax.rem(lax.div(self.place + 1, jnp.int32(2)), jnp.int32(2)) == 1

    def digit(self, axis, unit, base):
        return lax.rem(lax.div(self.me[axis], jnp.int32(unit)), jnp.int32(base))

    def device(self, label):
        if label == "m":
            return {"rep": self.me["rep"] + 2 * (3 - 2 * self.place)}
        axis, n = self.of[label]
        return {axis: self.me[axis] + (1 << n) - 2 * (1 << n) * self.bit[label]}


def tiled(rows, step, body):
    def run(i, carry):
        body(pl.ds(pl.multiple_of(i * step, step), step))
        return carry

    lax.fori_loop(0, rows // step, run, 0)


def step_of(rows, most):
    for step in range(most, 0, -1):
        if rows % step == 0 and step % 16 == 0:
            return step
    return rows


def layer_kernel(counts, tokens, gain, key_grad, weight, keys, token_grad, grads, *scratch):
    (x, gains, kg, normed, turned, full, own, th, kc, s1, r1, s2, r2, zs, zr, hs, hr, got, kacc, dn, kout, invs, flat,
     load_sem, out_sem, core_sem, one_sem, two_sem, low_sem, mid_sem, up_sem, a_sem, wx_sem, wl_sem, wm_sem, wc_sem,
     wo_sem) = scratch
    lab = Labels(counts)
    bit = lab.bit
    tokens_here, features = x.shape
    groups, _, _, part, wide = own.shape
    rows = 4 * part
    width = kg.shape[1]
    shard = lab.me["shard"]
    core = bit["c"]
    unit = rows // 8
    inner = lab.inner

    def local(src, dst, sem):
        return pltpu.make_async_copy(src, dst, sem)

    def remote(src, dst, sems, label):
        return pltpu.make_async_remote_copy(
            src_ref=src, dst_ref=dst, send_sem=sems.at[0], recv_sem=sems.at[1],
            device_id=lab.device(label), device_id_type=pl.DeviceIdType.MESH,
        )

    sent = []

    def send(copy, role=None):
        copy.start()
        sent.append((role, copy))

    loaded = []

    def once(load):
        if all(load is not other for other in loaded):
            loaded.append(load)
            load.wait()

    def only(role):
        return pl.when(inner if role == "inner" else jnp.logical_not(inner))

    third = tokens_here // 3
    loads = [local(tokens.at[pl.ds(n * third, third)], x.at[pl.ds(n * third, third)], load_sem.at[n]) for n in range(3)]
    load_gain = local(gain, gains, load_sem.at[3])
    load_kg = local(key_grad, kg, load_sem.at[4])
    load_w = local(weight, full.at[shard], load_sem.at[5])
    load_gain.start()
    for load in loads:
        load.start()
    load_kg.start()
    load_w.start()

    barrier = pltpu.get_barrier_semaphore()
    greeted = [*lab.of, "m"]
    for label in greeted:
        pl.semaphore_signal(barrier, inc=1, device_id=lab.device(label), device_id_type=pl.DeviceIdType.MESH)
    far = shard + 2 - 4 * bit["x"]
    near = shard + 1 - 2 * core
    both = far + 1 - 2 * core

    def rows_at(place):
        return (2 * place["x"] + place["c"]) * rows + (2 * place["y"] + place["l"]) * part

    tasks = {}

    arrived = []

    def weight_task(n, first, count):
        def at(place):
            return pl.ds(pl.multiple_of((first + place) * unit, 16), unit)

        def move(place, sems, label, shard_at=far):
            ref = full.at[shard_at, at(place)]
            return remote(ref, ref, sems, label)

        place = bit["l"] if count == 2 else lab.place
        beside = place + 1 - 2 * bit["l"]
        across, beyond = 3 - place, 3 - beside
        start = remote(weight.at[at(place)], full.at[shard, at(place)], wx_sem.at[n], "x")
        low = move(place, wl_sem.at[n, 0], "l")
        core0 = move(place, wc_sem.at[n, 0], "c")
        core1 = move(beside, wc_sem.at[n, 1], "c")
        arrived.extend([core0, core1])

        def wx():
            send(start)

        tasks[f"WX{n}"] = wx
        if count == 2:
            def wf():
                start.wait_recv()
                send(low)
                send(core0)

            def wg():
                low.wait_recv()
                send(core1)

            tasks[f"WF{n}"], tasks[f"WG{n}"] = wf, wg
            return

        mid0, mid1 = move(place, wm_sem.at[n, 0], "m"), move(beside, wm_sem.at[n, 1], "m")
        up1, up2 = move(across, wl_sem.at[n, 1], "l"), move(beyond, wl_sem.at[n, 2], "l")
        core_a, core_b = move(across, wc_sem.at[n, 2], "c"), move(beyond, wc_sem.at[n, 3], "c")
        end_a, end_b = move(beyond, wc_sem.at[n, 2], "c"), move(across, wc_sem.at[n, 3], "c")
        arrived.extend([core_a, core_b])

        def wf():
            start.wait_recv()
            send(low)

            @only("inner")
            def _():
                send(mid0, "inner")

            send(core0)

        def qa():
            low.wait_recv()

            @only("inner")
            def _():
                send(mid1, "inner")

            send(core1)

        def qb():
            @only("inner")
            def _():
                mid0.wait_recv()
                send(up1, "inner")
                send(core_a, "inner")

        def qc():
            @only("inner")
            def _():
                mid1.wait_recv()
                send(up2, "inner")
                send(core_b, "inner")

        def qd():
            @only("outer")
            def _():
                up1.wait_recv()
                send(end_a, "outer")

        def qe():
            @only("outer")
            def _():
                up2.wait_recv()
                send(end_b, "outer")

        for name, task in dict(WF=wf, QA=qa, QB=qb, QC=qc, QD=qd, QE=qe).items():
            tasks[f"{name}{n}"] = task

    first = 0
    for n, count in enumerate(SPREADS):
        weight_task(n, first, count)
        first += count
    assert first == 8
    own_copy = remote(full.at[shard], full.at[shard], wo_sem, "c")

    def weight_core():
        once(load_w)
        send(own_copy)

    tasks["WC"] = weight_core

    def gate():
        pl.semaphore_wait(barrier, len(greeted))

    tasks["GATE"] = gate

    def norm_task(n):
        def norm():
            if n == 0:
                load_gain.wait()
                flat[...] = jnp.concatenate([gains[k : k + 1, :] for k in range(features // gains.shape[1])], axis=1)
            loads[n].wait()

            def run(i, carry):
                at = pl.ds(pl.multiple_of(n * third + i * 16, 16), 16)
                value = x[at, :].astype(F32)
                inv = lax.rsqrt(jnp.mean(value * value, axis=1, keepdims=True) + 1e-06)
                invs[at, :] = inv
                normed[at, :] = (value * inv * flat[...]).astype(BF16)
                return carry

            lax.fori_loop(0, third // 16, run, 0, unroll=4)

        tasks[f"N{n}"] = norm

    def turn_task(name, half):
        def turn():
            for a in range(2):
                base = (2 * a + half) * rows

                def run(i, carry):
                    at = pl.ds(pl.multiple_of(base + i * 128, 128), 128)
                    turned[at, :] = normed[:, at].T
                    return carry

                lax.fori_loop(0, rows // 128, run, 0, unroll=3)

        tasks[name] = turn

    turn_task("RT", 1 - core)
    turn_task("RO", core)
    for n in range(3):
        norm_task(n)

    def outer(place, g):
        start = (2 * place["x"] + place["c"]) * rows + (2 * place["y"] + place["k"]) * part
        at = pl.ds(pl.multiple_of(start, 16), part)
        return jnp.dot(turned[at, :], kg[:, g * wide : (g + 1) * wide], preferred_element_type=F32)

    core_copies = [remote(th.at[g], kc.at[g], core_sem.at[g], "c") for g in range(groups)]

    def group_tasks(g):
        o1, o2 = HALVES[g]
        b1, b2 = bit[o1], bit[o2]
        def theirs():
            once(load_kg)

            def run(t, carry):
                a, b = t // 2, t % 2
                start = (2 * a + 1 - core) * rows + b * 2 * part
                at = pl.ds(pl.multiple_of(start, 16), 2 * part)
                total = jnp.dot(turned[at, :], kg[:, g * wide : (g + 1) * wide], preferred_element_type=F32)
                th[g, a, 2 * b] = total[:part].astype(BF16)
                th[g, a, 2 * b + 1] = total[part:].astype(BF16)
                return carry

            lax.fori_loop(0, 4, run, 0, unroll=2)
            send(core_copies[g])

        one = [[remote(s1.at[g, j, k], r1.at[g, j, k], one_sem.at[g, n, k], o1) for k in range(2)] for n, j in enumerate((1 - b2, b2))]

        def ours():
            core_copies[g].wait_recv()

            def piece(first, second, k):
                place = {o1: first, o2: second, "k": k, "c": core}
                came = kc[g, place["x"], 2 * place["y"] + k]
                return outer(place, g) + came.astype(F32)

            for n, j in enumerate((1 - b2, b2)):
                for k in range(2):
                    s1[g, j, k] = piece(1 - b1, j, k).astype(BF16)
                for k in range(2):
                    send(one[n][k])

            def keep(t, carry):
                own[g, t // 2, t % 2] = piece(b1, t // 2, t % 2)
                return carry

            lax.fori_loop(0, 4, keep, 0, unroll=2)

        tasks[f"T{g}"], tasks[f"O{g}"] = theirs, ours
        step = step_of(part, 96)
        arrivals = []

        def half_tasks(k):
            two = remote(s2.at[g, k], r2.at[g, k], two_sem.at[g, k], o2)
            low = remote(zs.at[g, k], zr.at[g, k], low_sem.at[g, k], "l")
            lanes = ["m", *lab.extra]
            mids = [remote(hs.at[g, k, n], hr.at[g, k, n], mid_sem.at[g, k, n], label) for n, label in enumerate(lanes)]
            mine = got.at[g, bit["y"], k]
            up = remote(mine, mine, up_sem.at[g, k], "l")
            last = remote(mine, mine, a_sem.at[g, k], "y")
            arrivals.append(last)

            def second():
                one[0][k].wait_recv()

                def add(at):
                    s2[g, k, at, :] = (own[g, 1 - b2, k, at, :] + r1[g, 1 - b2, k, at, :].astype(F32)).astype(BF16)

                tiled(part, step, add)
                send(two)

            def total(at):
                value = own[g, b2, k, at, :] + r1[g, b2, k, at, :].astype(F32)
                return value + r2[g, k, at, :].astype(F32)

            def third_step():
                @only("outer")
                def _():
                    one[1][k].wait_recv()
                    two.wait_recv()

                    def add(at):
                        zs[g, k, at, :] = total(at).astype(BF16)

                    tiled(part, step, add)
                    send(low, "outer")

            def fourth():
                @only("inner")
                def _():
                    one[1][k].wait_recv()
                    two.wait_recv()
                    low.wait_recv()

                    def add(at):
                        hs[g, k, 0, at, :] = (total(at) + zr[g, k, at, :].astype(F32)).astype(BF16)

                    tiled(part, step, add)
                    send(mids[0], "inner")

            def fifth():
                @only("inner")
                def _():
                    for n in range(len(mids)):
                        mids[n].wait_recv()

                        def add(at):
                            value = (hs[g, k, n, at, :].astype(F32) + hr[g, k, n, at, :].astype(F32)).astype(BF16)
                            if n + 1 == len(mids):
                                got[g, bit["y"], k, at, :] = value
                            else:
                                hs[g, k, n + 1, at, :] = value

                        tiled(part, step, add)
                        if n + 1 < len(mids):
                            send(mids[n + 1], "inner")
                    send(up, "inner")
                    send(last, "inner")

            def ends():
                @only("outer")
                def _():
                    up.wait_recv()
                    send(last, "outer")

            for name, task in dict(C2=second, C3=third_step, C4=fourth, C5=fifth, E5=ends).items():
                tasks[f"{name}{g}{k}"] = task

        for k in range(2):
            half_tasks(k)

        def seventh():
            for copy in arrivals:
                copy.wait_recv()
            for a in range(2):
                for k in range(2):
                    out = grads.at[2 * a + k, :, pl.ds(g * wide, wide)]
                    put(local(got.at[g, a, k], out, out_sem.at[g, 2 * a + k]))

        tasks[f"C7{g}"] = seventh

    written = []

    def put(copy):
        copy.start()
        written.append(copy)

    for g in range(groups):
        group_tasks(g)

    def forward(index, first):
        base = pl.multiple_of(index * rows, 128)

        def key_part(t, carry):
            at = pl.ds(pl.multiple_of(t * 256, 256), 256)
            total = jnp.dot(normed[:, pl.ds(base, rows)], full[index, :, at], preferred_element_type=F32)
            if first:
                kacc[:, at] = total
            else:
                kacc[:, at] += total
            return carry

        lax.fori_loop(0, width // 256, key_part, 0, unroll=2)

    def backward(index):
        base = pl.multiple_of(index * rows, 128)
        cut = 384

        def back_part(t, carry):
            at = pl.ds(pl.multiple_of(t * cut, 128), cut)
            to = pl.ds(pl.multiple_of(base + t * cut, 128), cut)
            dn[:, to] = lax.dot_general(
                kg[...], full[index, at, :], (((1,), (1,)), ((), ())), preferred_element_type=F32
            )
            return carry

        lax.fori_loop(0, rows // cut, back_part, 0)

    def own_forward():
        once(load_w)
        forward(shard, True)

    def own_backward():
        once(load_w)
        once(load_kg)
        backward(shard)

    def near_forward():
        own_copy.wait_recv()
        forward(near, False)

    def both_forward():
        for copy in arrived:
            copy.wait_recv()
        forward(both, False)

    tasks.update(
        KO=own_forward, BO=own_backward,
        KC=near_forward, BC=lambda: backward(near),
        KF=lambda: forward(far, False), BF=lambda: backward(far),
        KG=both_forward, BG=lambda: backward(both),
    )

    def finish_task(n):
        def finish():
            def run(i, carry):
                at = pl.ds(pl.multiple_of(n * third + i * 16, 16), 16)
                kout[at, :] = kacc[at, :].astype(BF16)
                value = x[at, :].astype(F32)
                inv = invs[at, :]
                scaled = dn[at, :] * flat[...]
                inner = jnp.mean(scaled * value, axis=1, keepdims=True)
                x[at, :] = (inv * scaled - value * (inv * inv * inv * inner)).astype(BF16)
                return carry

            lax.fori_loop(0, third // 16, run, 0, unroll=2)
            at = pl.ds(n * third, third)
            put(local(x.at[at], token_grad.at[at], out_sem.at[groups, n]))
            if n == 2:
                put(local(kout, keys, out_sem.at[groups, 3]))

        tasks[f"F{n}"] = finish

    for n in range(3):
        finish_task(n)

    assert sorted(ORDER) == sorted(tasks)
    for name in ORDER:
        tasks[name]()
    for copy in written:
        copy.wait()
    for role, copy in sent:
        if role is None:
            copy.wait_send()
    for role in ("inner", "outer"):
        @only(role)
        def _():
            for where, copy in sent:
                if where == role:
                    copy.wait_send()


def layer(counts, tokens, gain, key_grad, weight):
    count, features = tokens.shape
    width = key_grad.shape[1]
    rows = weight.shape[0]
    groups = len(HALVES)
    wide = width // groups
    part = rows // 4
    hops = 1 + bits_of(counts["rep"]) - 3
    lanes = 128
    any_space = pl.BlockSpec(memory_space=pl.ANY)
    dma = pltpu.SemaphoreType.DMA
    spreads = len(SPREADS)
    scratch = [
        pltpu.VMEM((count, features), BF16),
        pltpu.VMEM((features // lanes, lanes), F32),
        pltpu.VMEM((count, width), BF16),
        pltpu.VMEM((count, features), BF16),
        pltpu.VMEM((features, count), BF16),
        pltpu.VMEM((4, rows, width), BF16),
        pltpu.VMEM((groups, 2, 2, part, wide), F32),
        pltpu.VMEM((groups, 2, 4, part, wide), BF16),
        pltpu.VMEM((groups, 2, 4, part, wide), BF16),
        pltpu.VMEM((groups, 2, 2, part, wide), BF16),
        pltpu.VMEM((groups, 2, 2, part, wide), BF16),
        pltpu.VMEM((groups, 2, part, wide), BF16),
        pltpu.VMEM((groups, 2, part, wide), BF16),
        pltpu.VMEM((groups, 2, part, wide), BF16),
        pltpu.VMEM((groups, 2, part, wide), BF16),
        pltpu.VMEM((groups, 2, hops, part, wide), BF16),
        pltpu.VMEM((groups, 2, hops, part, wide), BF16),
        pltpu.VMEM((groups, 2, 2, part, wide), BF16),
        pltpu.VMEM((count, width), F32),
        pltpu.VMEM((count, features), F32),
        pltpu.VMEM((count, width), BF16),
        pltpu.VMEM((count, 1), F32),
        pltpu.VMEM((1, features), F32),
        dma((6,)),
        dma((groups + 1, 4)),
        dma((groups, 2)),
        dma((groups, 2, 2, 2)),
        dma((groups, 2, 2)),
        dma((groups, 2, 2)),
        dma((groups, 2, hops, 2)),
        dma((groups, 2, 2)),
        dma((groups, 2, 2)),
        dma((spreads, 2)),
        dma((spreads, 3, 2)),
        dma((spreads, 2, 2)),
        dma((spreads, 4, 2)),
        dma((2,)),
    ]
    keys, token_grad, grads = pl.pallas_call(
        functools.partial(layer_kernel, counts),
        in_specs=[any_space] * 4,
        out_specs=[any_space] * 3,
        out_shape=[
            jax.ShapeDtypeStruct((count, width), BF16),
            jax.ShapeDtypeStruct((count, features), BF16),
            jax.ShapeDtypeStruct((4, part, width), BF16),
        ],
        scratch_shapes=scratch,
        compiler_params=pltpu.CompilerParams(
            collective_id=0, has_side_effects=True, vmem_limit_bytes=67043328
        ),
        name="layer",
    )(tokens, gain.reshape(features // lanes, lanes), key_grad, weight)
    return keys, token_grad, grads.reshape(rows, width)


def requantize_kernel(
    chunks, sub, grads, m_code, m_exp, v_code, v_exp, keys_in, token_in,
    step, m_rel, m_scale, v_rel, v_scale, keys_out, token_out,
    units, tops, keys, token, sems,
):
    here, last = pl.program_id(0), pl.num_programs(0) - 1
    into = [pltpu.make_async_copy(token_in, token, sems.at[0]), pltpu.make_async_copy(keys_in, keys, sems.at[1])]
    back = [pltpu.make_async_copy(token, token_out, sems.at[2]), pltpu.make_async_copy(keys, keys_out, sems.at[3])]

    @pl.when(here == 0)
    def _():
        for copy in into:
            copy.start()

    rows, width = m_code.shape
    size = width // chunks
    unit_m = jnp.exp2(m_exp[...].astype(F32)) * (0.9 / 127.0)
    unit_v = jnp.exp2(v_exp[...].astype(F32)) * (0.999 / 255.0)
    units[...] = jnp.concatenate([unit_m, unit_v], axis=0).T
    floor = 1e-08 * bias_second**0.5
    rate = bias_second**0.5 / bias_first

    def run(i, carry):
        at = pl.ds(pl.multiple_of(i * sub, sub), sub)
        for c in range(chunks):
            cols = slice(c * size, (c + 1) * size)
            g = grads[at, cols].astype(F32)
            m_new = m_code[at, cols].astype(F32) * units[at, c : c + 1] + 0.1 * g
            v_new = v_code[at, cols].astype(F32) * units[at, chunks + c : chunks + c + 1] + 0.001 * g * g
            root = v_new * lax.rsqrt(v_new)
            step[at, cols] = (m_new * rate) / (root + floor)
            m_top = jnp.max(jnp.abs(m_new), axis=1, keepdims=True)
            v_top = jnp.max(v_new, axis=1, keepdims=True)
            tops[at, c : c + 1] = m_top
            tops[at, chunks + c : chunks + c + 1] = v_top
            m_rel[at, cols] = (m_new * (1.0 / (m_top + 1e-06))).astype(BF16)
            v_rel[at, cols] = (v_new * (1.0 / (v_top + 1e-06))).astype(BF16)
        return carry

    lax.fori_loop(0, rows // sub, run, 0, unroll=True)
    turned = tops[...].T
    m_scale[...] = turned[:chunks]
    v_scale[...] = turned[chunks:]

    @pl.when(here == last - 1)
    def _():
        for one, other in zip(into, back):
            one.wait()
            other.start()

    @pl.when(here == last)
    def _():
        for copy in back:
            copy.wait()


def requantize(grads, m_code, m_exp, v_code, v_exp, keys, token_grad, block=384, sub=128):
    rows, width = m_code.shape
    chunks = m_exp.shape[1]
    wide = pl.BlockSpec((block, width), lambda i: (i, 0))
    thin = pl.BlockSpec((chunks, block), lambda i: (0, i))
    any_space = pl.BlockSpec(memory_space=pl.ANY)
    shape = jax.ShapeDtypeStruct
    step, m_rel, m_scale, v_rel, v_scale, keys, token_grad = pl.pallas_call(
        functools.partial(requantize_kernel, chunks, sub),
        grid=(rows // block,),
        in_specs=[wide, wide, thin, wide, thin, any_space, any_space],
        out_specs=[wide, wide, thin, wide, thin, any_space, any_space],
        out_shape=[
            shape((rows, width), F32),
            shape((rows, width), BF16),
            shape((chunks, rows), F32),
            shape((rows, width), BF16),
            shape((chunks, rows), F32),
            shape(keys.shape, keys.dtype),
            shape(token_grad.shape, token_grad.dtype),
        ],
        scratch_shapes=[
            pltpu.VMEM((block, 2 * chunks), F32),
            pltpu.VMEM((block, 2 * chunks), F32),
            pltpu.VMEM(keys.shape, keys.dtype),
            pltpu.VMEM(token_grad.shape, token_grad.dtype),
            pltpu.SemaphoreType.DMA((4,)),
        ],
        name="requantize",
    )(grads, m_code, m_exp.T, v_code, v_exp.T, keys, token_grad)
    return keys, token_grad, step, m_rel, m_scale.T, v_rel, v_scale.T


def body(counts, tokens, norm_gain, key_grad, key_weight, m_code, m_exp, v_code, v_exp):
    keys, token_grad, grads = layer(counts, tokens, norm_gain, key_grad, key_weight)
    return requantize(grads, m_code, m_exp, v_code, v_exp, keys, token_grad)


def solution(mesh):
    rows = P("shard", None)
    tokens = P(("shard", "rep"), None)
    return jax.shard_map(
        functools.partial(body, dict(mesh.shape)),
        mesh=mesh,
        in_specs=(tokens, P(), tokens, rows, rows, rows, rows, rows),
        out_specs=(tokens, tokens, rows, rows, rows, rows, rows),
        check_vma=False,
    )
```

```python
import functools

import jax
import jax.numpy as jnp
from jax import lax
from jax.experimental import pallas as pl
from jax.experimental.pallas import tpu as pltpu
from jax.sharding import PartitionSpec as P

bias_first = 0.9999734386011124
bias_second = 0.0952078528862904
F32 = jnp.float32
BF16 = jnp.bfloat16

GROUPS = 4
CUTS = 3
HALVES = [
    "x", "y", "x", "x", "y", "y", "y", "x", "y", "y", "y", "y",
]
KINDS = ["core", "one", "two", "low", "mid", "up", "last", "far"]
SPREADS = [2, 2, 4]
ORDER = [
    "N0", "N1", "N2", "RT", "GATE", "WX0", "T.8", "T.6", "RO", "T.9", "WX2", "O.8", "T.4", "T.10", "O.9", "T.1",
    "T.3", "WF0", "T.11", "T.5", "O.11", "WX1", "O.6", "T.7", "T.2", "WF2", "C2.9", "WC", "C2.8", "T.0", "O.1",
    "WF1", "O.4", "C2.1", "O.3", "QB2", "O.7", "QA2", "BO", "C3.8", "C3.9", "O.5", "C2.3", "C4.8", "C2.5", "KO",
    "QC2", "C3.1", "O.2", "C2.7", "C3.3", "O.10", "C3.5", "WG0", "C5.8", "C4.1", "KC", "C2.4", "C2.2", "C2.11",
    "C3.7", "C4.9", "C4.5", "E5.8", "C2.10", "C5.1", "C4.7", "C5.9", "O.0", "QD2", "WG1", "C3.4", "QE2", "E5.1",
    "C3.2", "C5.5", "E5.9", "C4.3", "C3.11", "BC", "C5.7", "E5.5", "C7.8", "C4.4", "C4.2", "C3.10", "C2.6",
    "C5.4", "C4.11", "C2.0", "C5.3", "C7.1", "E5.7", "C7.9", "KG", "C4.10", "KF", "C3.0", "C5.11", "E5.4", "BF",
    "E5.3", "C3.6", "C5.2", "C7.4", "E5.11", "C4.0", "C7.7", "C5.10", "C7.5", "BG", "E5.2", "C4.6", "F0",
    "C7.3", "E5.10", "C5.0", "F1", "C7.11", "C5.6", "F2", "E5.0", "C7.2", "C7.10", "E5.6", "C7.0", "C7.6",
]


def bits_of(count):
    bits = count.bit_length() - 1
    assert 1 << bits == count
    return bits


class Labels:
    def __init__(self, counts):
        shards, reps = bits_of(counts["shard"]), bits_of(counts["rep"])
        assert shards == 2 and reps >= 3
        self.me = {axis: lax.axis_index(axis) for axis in ("shard", "rep")}
        self.of = {"c": ("shard", 0), "x": ("shard", 1), "y": ("rep", 0), "l": ("rep", 1)}
        self.extra = [f"h{n}" for n in range(3, reps)]
        for n in range(3, reps):
            self.of[f"h{n}"] = ("rep", n)
        self.bit = {label: self.digit(axis, 1 << n, 2) for label, (axis, n) in self.of.items()}
        self.place = self.digit("rep", 2, 4)
        self.inner = lax.rem(lax.div(self.place + 1, jnp.int32(2)), jnp.int32(2)) == 1

    def digit(self, axis, unit, base):
        return lax.rem(lax.div(self.me[axis], jnp.int32(unit)), jnp.int32(base))

    def device(self, label):
        if label == "m":
            return {"rep": self.me["rep"] + 2 * (3 - 2 * self.place)}
        axis, n = self.of[label]
        return {axis: self.me[axis] + (1 << n) - 2 * (1 << n) * self.bit[label]}


def tiled(rows, step, body):
    def run(i, carry):
        body(pl.ds(pl.multiple_of(i * step, step), step))
        return carry

    lax.fori_loop(0, rows // step, run, 0)


def step_of(rows, most):
    for step in range(most, 0, -1):
        if rows % step == 0 and step % 16 == 0:
            return step
    return rows


def layer_kernel(counts, tokens, gain, key_grad, weight, keys, token_grad, grads, *scratch):
    (x, gains, kg, normed, turned, full, own, th, kc, s1, r1, s2, r2, zr, hs, hr, got, kacc, dn, tg, kout, invs, flat,
     load_sem, out_sem, part_sem, send_sem, core_sem, one_sem, two_sem, low_sem, mid_sem, up_sem, a_sem, wx_sem, wl_sem, wm_sem, wc_sem,
     wo_sem) = scratch
    lab = Labels(counts)
    bit = lab.bit
    tokens_here, features = x.shape
    blocks, _, part, wide = own.shape
    rows = full.shape[1]
    width = kg.shape[1]
    shard = lab.me["shard"]
    core = bit["c"]
    unit = rows // 8
    inner = lab.inner

    def local(src, dst, sem):
        return pltpu.make_async_copy(src, dst, sem)

    def remote(src, dst, came, label, kind):
        return pltpu.make_async_remote_copy(
            src_ref=src, dst_ref=dst, send_sem=send_sem.at[KINDS.index(kind)], recv_sem=came,
            device_id=lab.device(label), device_id_type=pl.DeviceIdType.MESH,
        )

    sent = {None: 0, "inner": 0, "outer": 0}

    def send(copy, role=None, units=0):
        copy.start()
        sent[role] += units

    loaded = []

    def once(load):
        if all(load is not other for other in loaded):
            loaded.append(load)
            load.wait()

    def only(role):
        return pl.when(inner if role == "inner" else jnp.logical_not(inner))

    third = tokens_here // 3
    loads = [local(tokens.at[pl.ds(n * third, third)], x.at[pl.ds(n * third, third)], load_sem.at[n]) for n in range(3)]
    load_gain = local(gain, gains, load_sem.at[3])
    load_kg = local(key_grad, kg, load_sem.at[4])
    load_w = local(weight, full.at[shard], load_sem.at[5])
    load_gain.start()
    for load in loads:
        load.start()
    load_kg.start()
    load_w.start()

    barrier = pltpu.get_barrier_semaphore()
    greeted = [*lab.of, "m"]
    for label in greeted:
        pl.semaphore_signal(barrier, inc=1, device_id=lab.device(label), device_id_type=pl.DeviceIdType.MESH)
    far = shard + 2 - 4 * bit["x"]
    near = shard + 1 - 2 * core
    both = far + 1 - 2 * core

    def rows_at(place):
        return (2 * place["x"] + place["c"]) * rows + (2 * place["y"] + place["l"]) * part

    tasks = {}

    arrived = []

    def weight_task(n, first, count):
        def at(place):
            return pl.ds(pl.multiple_of((first + place) * unit, 16), unit)

        def move(place, sems, label, shard_at=far):
            ref = full.at[shard_at, at(place)]
            return remote(ref, ref, sems, label, "far")

        place = bit["l"] if count == 2 else lab.place
        beside = place + 1 - 2 * bit["l"]
        across, beyond = 3 - place, 3 - beside
        start = remote(weight.at[at(place)], full.at[shard, at(place)], wx_sem.at[n], "x", "far")
        low = move(place, wl_sem.at[n, 0], "l")
        core0 = move(place, wc_sem.at[n, 0], "c")
        core1 = move(beside, wc_sem.at[n, 1], "c")
        arrived.extend([core0, core1])

        def wx():
            send(start, None, 1)

        tasks[f"WX{n}"] = wx
        if count == 2:
            def wf():
                start.wait_recv()
                send(low, None, 1)
                send(core0, None, 1)

            def wg():
                low.wait_recv()
                send(core1, None, 1)

            tasks[f"WF{n}"], tasks[f"WG{n}"] = wf, wg
            return

        mid0, mid1 = move(place, wm_sem.at[n, 0], "m"), move(beside, wm_sem.at[n, 1], "m")
        up1, up2 = move(across, wl_sem.at[n, 1], "l"), move(beyond, wl_sem.at[n, 2], "l")
        core_a, core_b = move(across, wc_sem.at[n, 2], "c"), move(beyond, wc_sem.at[n, 3], "c")
        end_a, end_b = move(beyond, wc_sem.at[n, 2], "c"), move(across, wc_sem.at[n, 3], "c")
        arrived.extend([core_a, core_b])

        def wf():
            start.wait_recv()
            send(low, None, 1)

            @only("inner")
            def _():
                send(mid0, "inner", 1)

            send(core0, None, 1)

        def qa():
            low.wait_recv()

            @only("inner")
            def _():
                send(mid1, "inner", 1)

            send(core1, None, 1)

        def qb():
            @only("inner")
            def _():
                mid0.wait_recv()
                send(up1, "inner", 1)
                send(core_a, "inner", 1)

        def qc():
            @only("inner")
            def _():
                mid1.wait_recv()
                send(up2, "inner", 1)
                send(core_b, "inner", 1)

        def qd():
            @only("outer")
            def _():
                up1.wait_recv()
                send(end_a, "outer", 1)

        def qe():
            @only("outer")
            def _():
                up2.wait_recv()
                send(end_b, "outer", 1)

        for name, task in dict(WF=wf, QA=qa, QB=qb, QC=qc, QD=qd, QE=qe).items():
            tasks[f"{name}{n}"] = task

    first = 0
    for n, count in enumerate(SPREADS):
        weight_task(n, first, count)
        first += count
    assert first == 8
    own_copy = remote(full.at[shard], full.at[shard], wo_sem.at[0], "c", "far")

    def weight_core():
        once(load_w)
        send(own_copy, None, 8)

    tasks["WC"] = weight_core

    def gate():
        pl.semaphore_wait(barrier, len(greeted))

    tasks["GATE"] = gate

    def norm_task(n):
        def norm():
            if n == 0:
                load_gain.wait()
                flat[...] = jnp.concatenate([gains[k : k + 1, :] for k in range(features // gains.shape[1])], axis=1)
            loads[n].wait()

            def run(i, carry):
                at = pl.ds(pl.multiple_of(n * third + i * 16, 16), 16)
                value = x[at, :].astype(F32)
                inv = lax.rsqrt(jnp.mean(value * value, axis=1, keepdims=True) + 1e-06)
                invs[at, :] = inv
                normed[at, :] = (value * inv * flat[...]).astype(BF16)
                return carry

            lax.fori_loop(0, third // 16, run, 0, unroll=4)

        tasks[f"N{n}"] = norm

    def turn_task(name, half):
        def turn():
            for a in range(2):
                base = (2 * a + half) * rows

                def run(i, carry):
                    at = pl.ds(pl.multiple_of(base + i * 128, 128), 128)
                    turned[at, :] = normed[:, at].T
                    return carry

                lax.fori_loop(0, rows // 128, run, 0, unroll=3)

        tasks[name] = turn

    turn_task("RT", 1 - core)
    turn_task("RO", core)
    for n in range(3):
        norm_task(n)

    def outer(place, b):
        g, k = b // CUTS, b % CUTS
        start = (2 * place["x"] + place["c"]) * rows + (CUTS * place["y"] + k) * part
        at = pl.ds(pl.multiple_of(start, 16), part)
        return jnp.dot(turned[at, :], kg[:, g * wide : (g + 1) * wide], preferred_element_type=F32)

    step = step_of(part, 96)

    def block_tasks(b):
        o1 = HALVES[b]
        o2 = "y" if o1 == "x" else "x"
        b1, b2 = bit[o1], bit[o2]
        g, k = b // CUTS, b % CUTS
        over = remote(th.at[b], kc.at[b], core_sem.at[b], "c", "core")
        one = [remote(s1.at[b, j], r1.at[b, j], one_sem.at[b, n], o1, "one") for n, j in enumerate((1 - b2, b2))]
        two = remote(s2.at[b], r2.at[b], two_sem.at[b], o2, "two")
        low = remote(hs.at[b, 0], zr.at[b], low_sem.at[b], "l", "low")
        lanes = ["m", *lab.extra]
        mids = [remote(hs.at[b, n], hr.at[b, n], mid_sem.at[b, n], label, "mid") for n, label in enumerate(lanes)]
        mine = got.at[b, bit["y"]]
        up = remote(mine, mine, up_sem.at[b], "l", "up")
        last = remote(mine, mine, a_sem.at[b], "y", "last")

        def theirs():
            once(load_kg)
            for a in range(2):
                for y in range(2):
                    th[b, a, y] = outer({"x": a, "y": y, "c": 1 - core}, b).astype(BF16)
            send(over)

        def ours():
            over.wait_recv()

            def piece(first, second):
                place = {o1: first, o2: second, "c": core}
                return outer(place, b) + kc[b, place["x"], place["y"]].astype(F32)

            for n, j in enumerate((1 - b2, b2)):
                s1[b, j] = piece(1 - b1, j).astype(BF16)
                send(one[n])
            for j in range(2):
                own[b, j] = piece(b1, j)

        def second():
            one[0].wait_recv()

            def add(at):
                s2[b, at, :] = (own[b, 1 - b2, at, :] + r1[b, 1 - b2, at, :].astype(F32)).astype(BF16)

            tiled(part, step, add)
            send(two)

        def total(at):
            value = own[b, b2, at, :] + r1[b, b2, at, :].astype(F32)
            return value + r2[b, at, :].astype(F32)

        def third_step():
            @only("outer")
            def _():
                one[1].wait_recv()
                two.wait_recv()

                def add(at):
                    hs[b, 0, at, :] = total(at).astype(BF16)

                tiled(part, step, add)
                send(low, "outer")

        def fourth():
            @only("inner")
            def _():
                one[1].wait_recv()
                two.wait_recv()
                low.wait_recv()

                def add(at):
                    hs[b, 0, at, :] = (total(at) + zr[b, at, :].astype(F32)).astype(BF16)

                tiled(part, step, add)
                send(mids[0], "inner")

        def fifth():
            @only("inner")
            def _():
                for n in range(len(mids)):
                    mids[n].wait_recv()

                    def add(at):
                        value = (hs[b, n, at, :].astype(F32) + hr[b, n, at, :].astype(F32)).astype(BF16)
                        if n + 1 == len(mids):
                            got[b, bit["y"], at, :] = value
                        else:
                            hs[b, n + 1, at, :] = value

                    tiled(part, step, add)
                    if n + 1 < len(mids):
                        send(mids[n + 1], "inner")
                send(up, "inner")
                send(last, "inner")

        def ends():
            @only("outer")
            def _():
                up.wait_recv()
                send(last, "outer")

            finish_part(bit["y"])

        def finish_part(y):
            local(got.at[b, y], grads.at[CUTS * y + k, :, pl.ds(g * wide, wide)], part_sem.at[0]).start()

        def seventh():
            last.wait_recv()
            finish_part(1 - bit["y"])

        names = dict(T=theirs, O=ours, C2=second, C3=third_step, C4=fourth, C5=fifth, E5=ends, C7=seventh)
        for name, task in names.items():
            tasks[f"{name}.{b}"] = task

    written = []

    def put(copy):
        copy.start()
        written.append(copy)

    for b in range(blocks):
        block_tasks(b)

    def forward(index, first):
        base = pl.multiple_of(index * rows, 128)

        def key_part(t, carry):
            at = pl.ds(pl.multiple_of(t * 256, 256), 256)
            total = jnp.dot(normed[:, pl.ds(base, rows)], full[index, :, at], preferred_element_type=F32)
            if first:
                kacc[:, at] = total
            else:
                kacc[:, at] += total
            return carry

        lax.fori_loop(0, width // 256, key_part, 0, unroll=2)

    def backward(index):
        base = pl.multiple_of(index * rows, 128)
        cut = 384

        def back_part(t, carry):
            at = pl.ds(pl.multiple_of(t * cut, 128), cut)
            to = pl.ds(pl.multiple_of(base + t * cut, 128), cut)
            dn[:, to] = lax.dot_general(
                kg[...], full[index, at, :], (((1,), (1,)), ((), ())), preferred_element_type=F32
            )
            return carry

        lax.fori_loop(0, rows // cut, back_part, 0)

    def own_forward():
        once(load_w)
        forward(shard, True)

    def own_backward():
        once(load_w)
        once(load_kg)
        backward(shard)

    def near_forward():
        own_copy.wait_recv()
        forward(near, False)

    def both_forward():
        for copy in arrived:
            copy.wait_recv()
        forward(both, False)

    tasks.update(
        KO=own_forward, BO=own_backward,
        KC=near_forward, BC=lambda: backward(near),
        KF=lambda: forward(far, False), BF=lambda: backward(far),
        KG=both_forward, BG=lambda: backward(both),
    )

    def finish_task(n):
        def finish():
            def run(i, carry):
                at = pl.ds(pl.multiple_of(n * third + i * 16, 16), 16)
                value = x[at, :].astype(F32)
                inv = invs[at, :]
                scaled = dn[at, :] * flat[...]
                inner = jnp.mean(scaled * value, axis=1, keepdims=True)
                tg[at, :] = (inv * scaled - value * (inv * inv * inv * inner)).astype(BF16)
                return carry

            lax.fori_loop(0, third // 16, run, 0, unroll=2)
            at = pl.ds(n * third, third)
            put(local(tg.at[at], token_grad.at[at], out_sem.at[n]))
            if n == 2:
                kout[...] = kacc[...].astype(BF16)
                put(local(kout, keys, out_sem.at[3]))

        tasks[f"F{n}"] = finish

    for n in range(3):
        finish_task(n)

    assert sorted(ORDER) == sorted(tasks)
    for name in ORDER:
        tasks[name]()

    def left(kind, ref):
        local(ref, ref, send_sem.at[KINDS.index(kind)]).wait()

    def left_units(count):
        if count >= 8:
            left("far", full.at[pl.ds(0, count // 8)])
        if count % 8:
            left("far", full.at[0, pl.ds(0, count % 8 * unit)])

    half = got.at[pl.ds(0, blocks // 2)]
    for kind, ref in (("core", th), ("one", s1), ("two", s2), ("last", half)):
        left(kind, ref)
    left_units(sent[None])

    @only("inner")
    def _():
        left("mid", hs)
        left("up", half)
        left_units(sent["inner"])

    @only("outer")
    def _():
        left("low", hs.at[:, 0])
        left_units(sent["outer"])

    local(got, got, part_sem.at[0]).wait()
    for copy in written:
        copy.wait()


def layer(counts, tokens, gain, key_grad, weight):
    count, features = tokens.shape
    width = key_grad.shape[1]
    rows = weight.shape[0]
    blocks = len(HALVES)
    assert blocks == GROUPS * CUTS
    wide = width // GROUPS
    part = rows // (2 * CUTS)
    hops = 1 + bits_of(counts["rep"]) - 3
    lanes = 128
    any_space = pl.BlockSpec(memory_space=pl.ANY)
    dma = pltpu.SemaphoreType.DMA
    spreads = len(SPREADS)
    scratch = [
        pltpu.VMEM((count, features), BF16),
        pltpu.VMEM((features // lanes, lanes), F32),
        pltpu.VMEM((count, width), BF16),
        pltpu.VMEM((count, features), BF16),
        pltpu.VMEM((features, count), BF16),
        pltpu.VMEM((4, rows, width), BF16),
        pltpu.VMEM((blocks, 2, part, wide), F32),
        pltpu.VMEM((blocks, 2, 2, part, wide), BF16),
        pltpu.VMEM((blocks, 2, 2, part, wide), BF16),
        pltpu.VMEM((blocks, 2, part, wide), BF16),
        pltpu.VMEM((blocks, 2, part, wide), BF16),
        pltpu.VMEM((blocks, part, wide), BF16),
        pltpu.VMEM((blocks, part, wide), BF16),
        pltpu.VMEM((blocks, part, wide), BF16),
        pltpu.VMEM((blocks, hops, part, wide), BF16),
        pltpu.VMEM((blocks, hops, part, wide), BF16),
        pltpu.VMEM((blocks, 2, part, wide), BF16),
        pltpu.VMEM((count, width), F32),
        pltpu.VMEM((count, features), F32),
        pltpu.VMEM((count, features), BF16),
        pltpu.VMEM((count, width), BF16),
        pltpu.VMEM((count, 1), F32),
        pltpu.VMEM((1, features), F32),
        dma((6,)),
        dma((4,)),
        dma((1,)),
        dma((len(KINDS),)),
        dma((blocks,)),
        dma((blocks, 2)),
        dma((blocks,)),
        dma((blocks,)),
        dma((blocks, hops)),
        dma((blocks,)),
        dma((blocks,)),
        dma((spreads,)),
        dma((spreads, 3)),
        dma((spreads, 2)),
        dma((spreads, 4)),
        dma((1,)),
    ]
    keys, token_grad, grads = pl.pallas_call(
        functools.partial(layer_kernel, counts),
        in_specs=[any_space] * 4,
        out_specs=[any_space] * 3,
        out_shape=[
            jax.ShapeDtypeStruct((count, width), BF16),
            jax.ShapeDtypeStruct((count, features), BF16),
            jax.ShapeDtypeStruct((2 * CUTS, part, width), BF16),
        ],
        scratch_shapes=scratch,
        compiler_params=pltpu.CompilerParams(
            collective_id=0, has_side_effects=True, vmem_limit_bytes=67043328
        ),
        name="layer",
    )(tokens, gain.reshape(features // lanes, lanes), key_grad, weight)
    return keys, token_grad, grads.reshape(rows, width)


def requantize_kernel(
    chunks, sub, grads, m_code, m_exp, v_code, v_exp, keys_in, token_in,
    step, m_rel, m_scale, v_rel, v_scale, keys_out, token_out,
    units, tops, keys, token, sems,
):
    here, last = pl.program_id(0), pl.num_programs(0) - 1
    into = [pltpu.make_async_copy(token_in, token, sems.at[0]), pltpu.make_async_copy(keys_in, keys, sems.at[1])]
    back = [pltpu.make_async_copy(token, token_out, sems.at[2]), pltpu.make_async_copy(keys, keys_out, sems.at[3])]

    @pl.when(here == 0)
    def _():
        for copy in into:
            copy.start()

    rows, width = m_code.shape
    size = width // chunks
    unit_m = jnp.exp2(m_exp[...].astype(F32)) * (0.9 / 127.0)
    unit_v = jnp.exp2(v_exp[...].astype(F32)) * (0.999 / 255.0)
    units[...] = jnp.concatenate([unit_m, unit_v], axis=0).T
    floor = 1e-08 * bias_second**0.5
    rate = bias_second**0.5 / bias_first

    def run(i, carry):
        at = pl.ds(pl.multiple_of(i * sub, sub), sub)
        for c in range(chunks):
            cols = slice(c * size, (c + 1) * size)
            g = grads[at, cols].astype(F32)
            m_new = m_code[at, cols].astype(F32) * units[at, c : c + 1] + 0.1 * g
            v_new = v_code[at, cols].astype(F32) * units[at, chunks + c : chunks + c + 1] + 0.001 * g * g
            root = v_new * lax.rsqrt(v_new)
            step[at, cols] = (m_new * rate) / (root + floor)
            m_top = jnp.max(jnp.abs(m_new), axis=1, keepdims=True)
            v_top = jnp.max(v_new, axis=1, keepdims=True)
            tops[at, c : c + 1] = m_top
            tops[at, chunks + c : chunks + c + 1] = v_top
            m_rel[at, cols] = (m_new * (1.0 / (m_top + 1e-06))).astype(BF16)
            v_rel[at, cols] = (v_new * (1.0 / (v_top + 1e-06))).astype(BF16)
        return carry

    lax.fori_loop(0, rows // sub, run, 0, unroll=True)
    turned = tops[...].T
    m_scale[...] = turned[:chunks]
    v_scale[...] = turned[chunks:]

    @pl.when(here == last - 1)
    def _():
        for one, other in zip(into, back):
            one.wait()
            other.start()

    @pl.when(here == last)
    def _():
        for copy in back:
            copy.wait()


def requantize(grads, m_code, m_exp, v_code, v_exp, keys, token_grad, block=384, sub=128):
    rows, width = m_code.shape
    chunks = m_exp.shape[1]
    wide = pl.BlockSpec((block, width), lambda i: (i, 0))
    thin = pl.BlockSpec((chunks, block), lambda i: (0, i))
    any_space = pl.BlockSpec(memory_space=pl.ANY)
    shape = jax.ShapeDtypeStruct
    step, m_rel, m_scale, v_rel, v_scale, keys, token_grad = pl.pallas_call(
        functools.partial(requantize_kernel, chunks, sub),
        grid=(rows // block,),
        in_specs=[wide, wide, thin, wide, thin, any_space, any_space],
        out_specs=[wide, wide, thin, wide, thin, any_space, any_space],
        out_shape=[
            shape((rows, width), F32),
            shape((rows, width), BF16),
            shape((chunks, rows), F32),
            shape((rows, width), BF16),
            shape((chunks, rows), F32),
            shape(keys.shape, keys.dtype),
            shape(token_grad.shape, token_grad.dtype),
        ],
        scratch_shapes=[
            pltpu.VMEM((block, 2 * chunks), F32),
            pltpu.VMEM((block, 2 * chunks), F32),
            pltpu.VMEM(keys.shape, keys.dtype),
            pltpu.VMEM(token_grad.shape, token_grad.dtype),
            pltpu.SemaphoreType.DMA((4,)),
        ],
        name="requantize",
    )(grads, m_code, m_exp.T, v_code, v_exp.T, keys, token_grad)
    return keys, token_grad, step, m_rel, m_scale.T, v_rel, v_scale.T


def body(counts, tokens, norm_gain, key_grad, key_weight, m_code, m_exp, v_code, v_exp):
    keys, token_grad, grads = layer(counts, tokens, norm_gain, key_grad, key_weight)
    return requantize(grads, m_code, m_exp, v_code, v_exp, keys, token_grad)


def solution(mesh):
    rows = P("shard", None)
    tokens = P(("shard", "rep"), None)
    return jax.shard_map(
        functools.partial(body, dict(mesh.shape)),
        mesh=mesh,
        in_specs=(tokens, P(), tokens, rows, rows, rows, rows, rows),
        out_specs=(tokens, tokens, rows, rows, rows, rows, rows),
        check_vma=False,
    )
```

```python
import functools

import jax
import jax.numpy as jnp
from jax import lax
from jax.experimental import pallas as pl
from jax.experimental.pallas import tpu as pltpu
from jax.sharding import PartitionSpec as P

bias_first = 0.9999734386011124
bias_second = 0.0952078528862904
F32 = jnp.float32
BF16 = jnp.bfloat16

GROUPS = 4
CUTS = 3
HALVES = [
    "x", "x", "y", "z", "y", "x", "y", "y", "y", "y", "y", "y",
]
KINDS = ["core", "one", "two", "low", "mid", "up", "last", "far"]
SPREADS = [2, 4, 2]
ORDER = [
    "N0", "N1", "N2", "GATE", "WX1", "RT", "T.11", "T.7", "T.10", "RO", "WX2", "O.11", "WX0", "O.7", "WF1",
    "T.4", "T.2", "T.0", "T.3", "T.8", "O.4", "C2.11", "C2.7", "O.10", "T.9", "O.0", "WF2", "T.1", "WC", "O.8",
    "T.5", "QA1", "O.2", "QB1", "C3.11", "C3.7", "T.6", "WF0", "C2.0", "C2.8", "C4.7", "O.9", "O.5", "QC1",
    "C4.11", "KO", "C2.10", "C5.7", "KC", "C2.5", "C3.8", "C5.11", "QD1", "BC", "C2.2", "C3.0", "C3.10", "C2.9",
    "C2.4", "O.3", "C3.5", "C4.8", "WG0", "C4.0", "C4.10", "WG2", "O.6", "C3.9", "BO", "C5.0", "C3.2", "C5.8",
    "C4.5", "C4.9", "C5.10", "E5.7", "QE1", "C2.6", "C3.4", "E5.11", "O.1", "KF", "D2.3", "C4.2", "C5.5",
    "E5.0", "KG", "D3.3", "E5.8", "C7.7", "C7.11", "BG", "C7.0", "C2.1", "C5.2", "D4.3", "C3.6", "E5.10",
    "C4.4", "BF", "C4.6", "E5.2", "C3.1", "D5.3", "C7.8", "C5.9", "F0", "C5.4", "F1", "E5.5", "C4.1", "F2",
    "C5.6", "C7.2", "C5.1", "C7.10", "D6.3", "E5.9", "E5.4", "E5.6", "D7.3", "C7.9", "E5.1", "C7.5", "C7.4",
    "C7.6", "D8.3", "C7.1",
]


def bits_of(count):
    bits = count.bit_length() - 1
    assert 1 << bits == count
    return bits


class Labels:
    def __init__(self, counts):
        shards, reps = bits_of(counts["shard"]), bits_of(counts["rep"])
        assert shards == 2 and reps >= 3
        self.me = {axis: lax.axis_index(axis) for axis in ("shard", "rep")}
        self.of = {"c": ("shard", 0), "x": ("shard", 1), "y": ("rep", 0), "l": ("rep", 1)}
        self.extra = [f"h{n}" for n in range(3, reps)]
        for n in range(3, reps):
            self.of[f"h{n}"] = ("rep", n)
        self.bit = {label: self.digit(axis, 1 << n, 2) for label, (axis, n) in self.of.items()}
        self.place = self.digit("rep", 2, 4)
        self.side = lax.div(self.place, jnp.int32(2))
        self.inner = lax.rem(lax.div(self.place + 1, jnp.int32(2)), jnp.int32(2)) == 1

    def digit(self, axis, unit, base):
        return lax.rem(lax.div(self.me[axis], jnp.int32(unit)), jnp.int32(base))

    def device(self, label):
        if label == "m":
            return {"rep": self.me["rep"] + 2 * (3 - 2 * self.place)}
        axis, n = self.of[label]
        return {axis: self.me[axis] + (1 << n) - 2 * (1 << n) * self.bit[label]}


def tiled(rows, step, body):
    def run(i, carry):
        body(pl.ds(pl.multiple_of(i * step, step), step))
        return carry

    lax.fori_loop(0, rows // step, run, 0)


def step_of(rows, most):
    for step in range(most, 0, -1):
        if rows % step == 0 and step % 16 == 0:
            return step
    return rows


def layer_kernel(counts, tokens, gain, key_grad, weight, keys, token_grad, grads, *scratch):
    (x, gains, kg, normed, turned, full, own, th, kc, s1, r1, s2, r2, zr, hs, hr, got, kacc, dn, tg, invs, flat,
     load_sem, out_sem, part_sem, send_sem, core_sem, one_sem, two_sem, low_sem, mid_sem, up_sem, a_sem, wx_sem, wl_sem, wm_sem, wc_sem,
     wo_sem) = scratch
    lab = Labels(counts)
    bit = lab.bit
    tokens_here, features = x.shape
    blocks, _, part, wide = own.shape
    rows = full.shape[1]
    width = kg.shape[1]
    shard = lab.me["shard"]
    core = bit["c"]
    unit = rows // 8
    inner = lab.inner

    def local(src, dst, sem):
        return pltpu.make_async_copy(src, dst, sem)

    def remote(src, dst, came, label, kind):
        return pltpu.make_async_remote_copy(
            src_ref=src, dst_ref=dst, send_sem=send_sem.at[KINDS.index(kind)], recv_sem=came,
            device_id=lab.device(label), device_id_type=pl.DeviceIdType.MESH,
        )

    sent = {None: 0, "inner": 0, "outer": 0}

    def send(copy, role=None, units=0):
        copy.start()
        sent[role] += units

    loaded = []

    def once(load):
        if all(load is not other for other in loaded):
            loaded.append(load)
            load.wait()

    def only(role):
        return pl.when(inner if role == "inner" else jnp.logical_not(inner))

    third = tokens_here // 3
    loads = [local(tokens.at[pl.ds(n * third, third)], x.at[pl.ds(n * third, third)], load_sem.at[n]) for n in range(3)]
    load_gain = local(gain, gains, load_sem.at[3])
    load_kg = local(key_grad, kg, load_sem.at[4])
    load_w = local(weight, full.at[shard], load_sem.at[5])
    load_gain.start()
    for load in loads:
        load.start()
    load_kg.start()
    load_w.start()

    barrier = pltpu.get_barrier_semaphore()
    greeted = [*lab.of, "m"]
    for label in greeted:
        pl.semaphore_signal(barrier, inc=1, device_id=lab.device(label), device_id_type=pl.DeviceIdType.MESH)
    far = shard + 2 - 4 * bit["x"]
    near = shard + 1 - 2 * core
    both = far + 1 - 2 * core

    def rows_at(place):
        return (2 * place["x"] + place["c"]) * rows + (2 * place["y"] + place["l"]) * part

    tasks = {}

    arrived = []

    def weight_task(n, first, count):
        def at(place):
            return pl.ds(pl.multiple_of((first + place) * unit, 16), unit)

        def move(place, sems, label, shard_at=far):
            ref = full.at[shard_at, at(place)]
            return remote(ref, ref, sems, label, "far")

        place = bit["l"] if count == 2 else lab.place
        beside = place + 1 - 2 * bit["l"]
        across, beyond = 3 - place, 3 - beside
        start = remote(weight.at[at(place)], full.at[shard, at(place)], wx_sem.at[n], "x", "far")
        low = move(place, wl_sem.at[n, 0], "l")
        core0 = move(place, wc_sem.at[n, 0], "c")
        core1 = move(beside, wc_sem.at[n, 1], "c")
        arrived.extend([core0, core1])

        def wx():
            send(start, None, 1)

        tasks[f"WX{n}"] = wx
        if count == 2:
            def wf():
                start.wait_recv()
                send(low, None, 1)
                send(core0, None, 1)

            def wg():
                low.wait_recv()
                send(core1, None, 1)

            tasks[f"WF{n}"], tasks[f"WG{n}"] = wf, wg
            return

        mid0, mid1 = move(place, wm_sem.at[n, 0], "m"), move(beside, wm_sem.at[n, 1], "m")
        up1, up2 = move(across, wl_sem.at[n, 1], "l"), move(beyond, wl_sem.at[n, 2], "l")
        core_a, core_b = move(across, wc_sem.at[n, 2], "c"), move(beyond, wc_sem.at[n, 3], "c")
        end_a, end_b = move(beyond, wc_sem.at[n, 2], "c"), move(across, wc_sem.at[n, 3], "c")
        arrived.extend([core_a, core_b])

        def wf():
            start.wait_recv()
            send(low, None, 1)

            @only("inner")
            def _():
                send(mid0, "inner", 1)

            send(core0, None, 1)

        def qa():
            low.wait_recv()

            @only("inner")
            def _():
                send(mid1, "inner", 1)

            send(core1, None, 1)

        def qb():
            @only("inner")
            def _():
                mid0.wait_recv()
                send(up1, "inner", 1)
                send(core_a, "inner", 1)

        def qc():
            @only("inner")
            def _():
                mid1.wait_recv()
                send(up2, "inner", 1)
                send(core_b, "inner", 1)

        def qd():
            @only("outer")
            def _():
                up1.wait_recv()
                send(end_a, "outer", 1)

        def qe():
            @only("outer")
            def _():
                up2.wait_recv()
                send(end_b, "outer", 1)

        for name, task in dict(WF=wf, QA=qa, QB=qb, QC=qc, QD=qd, QE=qe).items():
            tasks[f"{name}{n}"] = task

    first = 0
    for n, count in enumerate(SPREADS):
        weight_task(n, first, count)
        first += count
    assert first == 8
    own_copy = remote(full.at[shard], full.at[shard], wo_sem.at[0], "c", "far")

    def weight_core():
        once(load_w)
        send(own_copy, None, 8)

    tasks["WC"] = weight_core

    def gate():
        pl.semaphore_wait(barrier, len(greeted))

    tasks["GATE"] = gate

    def norm_task(n):
        def norm():
            if n == 0:
                load_gain.wait()
                flat[...] = jnp.concatenate([gains[k : k + 1, :] for k in range(features // gains.shape[1])], axis=1)
            loads[n].wait()

            def run(i, carry):
                at = pl.ds(pl.multiple_of(n * third + i * 16, 16), 16)
                value = x[at, :].astype(F32)
                inv = lax.rsqrt(jnp.mean(value * value, axis=1, keepdims=True) + 1e-06)
                invs[at, :] = inv
                normed[at, :] = (value * inv * flat[...]).astype(BF16)
                return carry

            lax.fori_loop(0, third // 16, run, 0, unroll=4)

        tasks[f"N{n}"] = norm

    def turn_task(name, half):
        def turn():
            for a in range(2):
                base = (2 * a + half) * rows

                def run(i, carry):
                    at = pl.ds(pl.multiple_of(base + i * 128, 128), 128)
                    turned[at, :] = normed[:, at].T
                    return carry

                lax.fori_loop(0, rows // 128, run, 0, unroll=3)

        tasks[name] = turn

    turn_task("RT", 1 - core)
    turn_task("RO", core)
    for n in range(3):
        norm_task(n)

    def outer(place, b):
        g, k = b // CUTS, b % CUTS
        start = (2 * place["x"] + place["c"]) * rows + (CUTS * place["y"] + k) * part
        at = pl.ds(pl.multiple_of(start, 16), part)
        return jnp.dot(turned[at, :], kg[:, g * wide : (g + 1) * wide], preferred_element_type=F32)

    step = step_of(part, 96)

    def late_tasks(b, one, out_at, finish_part):
        e = blocks + HALVES[:b].count("z")
        second = lab.side
        spots = (1 - second, second)
        stores = (b, e)
        lanes = ["y", *lab.extra]
        lows = [remote(hs.at[s, 0], zr.at[s], low_sem.at[s], "l", "low") for s in stores]
        over = remote(hs.at[b, 0], hr.at[b, 0], mid_sem.at[b, 0], "m", "mid")
        chain = [remote(hs.at[e, n], hr.at[e, n], mid_sem.at[e, n], label, "mid") for n, label in enumerate(lanes)]
        mine, other = got.at[b, second], got.at[b, 1 - second]
        back = remote(mine, mine, a_sem.at[b], "m", "mid")
        ups = [remote(mine, out_at(second), up_sem.at[b], "l", "up"), remote(other, out_at(1 - second), up_sem.at[e], "l", "up")]

        def total(n, at):
            return own[b, spots[n], at, :] + r1[b, spots[n], at, :].astype(F32)

        def down(n):
            @only("outer")
            def _():
                one[n].wait_recv()

                def add(at):
                    hs[stores[n], 0, at, :] = total(n, at).astype(BF16)

                tiled(part, step, add)
                send(lows[n], "outer")

        def fourth():
            @only("inner")
            def _():
                one[0].wait_recv()
                lows[0].wait_recv()

                def add(at):
                    hs[b, 0, at, :] = (total(0, at) + zr[b, at, :].astype(F32)).astype(BF16)

                tiled(part, step, add)
                send(over, "inner")

        def fifth():
            @only("inner")
            def _():
                one[1].wait_recv()
                lows[1].wait_recv()
                over.wait_recv()

                def add(at):
                    value = total(1, at) + zr[e, at, :].astype(F32)
                    hs[e, 0, at, :] = (value + hr[b, 0, at, :].astype(F32)).astype(BF16)

                tiled(part, step, add)
                send(chain[0], "inner")

        def sixth():
            @only("inner")
            def _():
                for n in range(len(chain)):
                    chain[n].wait_recv()

                    def add(at):
                        value = (hs[e, n, at, :].astype(F32) + hr[e, n, at, :].astype(F32)).astype(BF16)
                        if n + 1 == len(chain):
                            got[b, second, at, :] = value
                        else:
                            hs[e, n + 1, at, :] = value

                    tiled(part, step, add)
                    if n + 1 < len(chain):
                        send(chain[n + 1], "inner")
                send(back, "inner")
                send(ups[0], "inner")
                finish_part(second)

        def seventh():
            @only("inner")
            def _():
                back.wait_recv()
                send(ups[1], "inner")
                finish_part(1 - second)

        def eighth():
            @only("outer")
            def _():
                for copy in ups:
                    copy.wait_recv()

        return dict(D2=lambda: down(0), D3=lambda: down(1), D4=fourth, D5=fifth, D6=sixth, D7=seventh, D8=eighth)

    def block_tasks(b):
        late = HALVES[b] == "z"
        o1 = "y" if HALVES[b] == "y" else "x"
        o2 = "x" if o1 == "y" else "y"
        b1 = bit[o1]
        b2 = lab.side if late else bit[o2]
        g, k = b // CUTS, b % CUTS
        def out_at(y):
            return grads.at[CUTS * y + k, :, pl.ds(g * wide, wide)]

        over = remote(th.at[b], kc.at[b], core_sem.at[b], "c", "core")
        one = [remote(s1.at[b, j], r1.at[b, j], one_sem.at[b, n], o1, "one") for n, j in enumerate((1 - b2, b2))]
        two = remote(s2.at[b], r2.at[b], two_sem.at[b], o2, "two")
        low = remote(hs.at[b, 0], zr.at[b], low_sem.at[b], "l", "low")
        lanes = ["m", *lab.extra]
        mids = [remote(hs.at[b, n], hr.at[b, n], mid_sem.at[b, n], label, "mid") for n, label in enumerate(lanes)]
        mine = got.at[b, bit["y"]]
        up = remote(mine, mine, up_sem.at[b], "l", "up")
        last = remote(mine, out_at(bit["y"]), a_sem.at[b], "y", "last")

        def theirs():
            once(load_kg)
            for a in range(2):
                for y in range(2):
                    th[b, a, y] = outer({"x": a, "y": y, "c": 1 - core}, b).astype(BF16)
            send(over)

        def ours():
            over.wait_recv()

            def piece(first, second):
                place = {o1: first, o2: second, "c": core}
                return outer(place, b) + kc[b, place["x"], place["y"]].astype(F32)

            for n, j in enumerate((1 - b2, b2)):
                s1[b, j] = piece(1 - b1, j).astype(BF16)
                send(one[n])
            for j in range(2):
                own[b, j] = piece(b1, j)

        def second():
            one[0].wait_recv()

            def add(at):
                s2[b, at, :] = (own[b, 1 - b2, at, :] + r1[b, 1 - b2, at, :].astype(F32)).astype(BF16)

            tiled(part, step, add)
            send(two)

        def total(at):
            value = own[b, b2, at, :] + r1[b, b2, at, :].astype(F32)
            return value + r2[b, at, :].astype(F32)

        def third_step():
            @only("outer")
            def _():
                one[1].wait_recv()
                two.wait_recv()

                def add(at):
                    hs[b, 0, at, :] = total(at).astype(BF16)

                tiled(part, step, add)
                send(low, "outer")

        def fourth():
            @only("inner")
            def _():
                one[1].wait_recv()
                two.wait_recv()
                low.wait_recv()

                def add(at):
                    hs[b, 0, at, :] = (total(at) + zr[b, at, :].astype(F32)).astype(BF16)

                tiled(part, step, add)
                send(mids[0], "inner")

        def fifth():
            @only("inner")
            def _():
                for n in range(len(mids)):
                    mids[n].wait_recv()

                    def add(at):
                        value = (hs[b, n, at, :].astype(F32) + hr[b, n, at, :].astype(F32)).astype(BF16)
                        if n + 1 == len(mids):
                            got[b, bit["y"], at, :] = value
                        else:
                            hs[b, n + 1, at, :] = value

                    tiled(part, step, add)
                    if n + 1 < len(mids):
                        send(mids[n + 1], "inner")
                send(up, "inner")
                send(last, "inner")

        def ends():
            @only("outer")
            def _():
                up.wait_recv()
                send(last, "outer")

            finish_part(bit["y"])

        def finish_part(y):
            local(got.at[b, y], out_at(y), part_sem.at[0]).start()

        def seventh():
            last.wait_recv()

        if late:
            names = dict(T=theirs, O=ours, **late_tasks(b, one, out_at, finish_part))
        else:
            names = dict(T=theirs, O=ours, C2=second, C3=third_step, C4=fourth, C5=fifth, E5=ends, C7=seventh)
        for name, task in names.items():
            tasks[f"{name}.{b}"] = task

    written = []

    def put(copy):
        copy.start()
        written.append(copy)

    for b in range(blocks):
        block_tasks(b)

    def forward(index, first):
        base = pl.multiple_of(index * rows, 128)

        def key_part(t, carry):
            at = pl.ds(pl.multiple_of(t * 256, 256), 256)
            total = jnp.dot(normed[:, pl.ds(base, rows)], full[index, :, at], preferred_element_type=F32)
            if first:
                kacc[:, at] = total
            else:
                kacc[:, at] += total
            return carry

        lax.fori_loop(0, width // 256, key_part, 0, unroll=2)

    def backward(index):
        base = pl.multiple_of(index * rows, 128)
        cut = 384

        def back_part(t, carry):
            at = pl.ds(pl.multiple_of(t * cut, 128), cut)
            to = pl.ds(pl.multiple_of(base + t * cut, 128), cut)
            dn[:, to] = lax.dot_general(
                kg[...], full[index, at, :], (((1,), (1,)), ((), ())), preferred_element_type=F32
            )
            return carry

        lax.fori_loop(0, rows // cut, back_part, 0)

    def own_forward():
        once(load_w)
        forward(shard, True)

    def own_backward():
        once(load_w)
        once(load_kg)
        backward(shard)

    def near_forward():
        own_copy.wait_recv()
        forward(near, False)

    def both_forward():
        for copy in arrived:
            copy.wait_recv()
        forward(both, False)

    tasks.update(
        KO=own_forward, BO=own_backward,
        KC=near_forward, BC=lambda: backward(near),
        KF=lambda: forward(far, False), BF=lambda: backward(far),
        KG=both_forward, BG=lambda: backward(both),
    )

    def finish_task(n):
        def finish():
            def run(i, carry):
                at = pl.ds(pl.multiple_of(n * third + i * 16, 16), 16)
                value = x[at, :].astype(F32)
                inv = invs[at, :]
                scaled = dn[at, :] * flat[...]
                inner = jnp.mean(scaled * value, axis=1, keepdims=True)
                tg[at, :] = (inv * scaled - value * (inv * inv * inv * inner)).astype(BF16)
                return carry

            lax.fori_loop(0, third // 16, run, 0, unroll=2)
            at = pl.ds(n * third, third)
            put(local(tg.at[at], token_grad.at[at], out_sem.at[n]))
            if n == 2:
                assert all(ORDER.index(f"O.{b}") < ORDER.index("F2") for b in range(blocks))
                kg[...] = kacc[...].astype(BF16)
                put(local(kg, keys, out_sem.at[3]))

        tasks[f"F{n}"] = finish

    for n in range(3):
        finish_task(n)

    assert sorted(ORDER) == sorted(tasks)
    for name in ORDER:
        tasks[name]()

    def left(kind, ref):
        local(ref, ref, send_sem.at[KINDS.index(kind)]).wait()

    def left_units(count):
        if count >= 8:
            left("far", full.at[pl.ds(0, count // 8)])
        if count % 8:
            left("far", full.at[0, pl.ds(0, count % 8 * unit)])

    def left_pieces(sem, count):
        while count > 0:
            take = min(count, 2 * blocks)
            for ref in ([s1.at[pl.ds(0, take // 2)]] if take > 1 else []) + ([s1.at[0, 0]] if take % 2 else []):
                local(ref, ref, sem).wait()
            count -= take

    def left_kind(kind, count):
        left_pieces(send_sem.at[KINDS.index(kind)], count)

    twice = HALVES.count("z")
    once_only = blocks - twice
    hops = hs.shape[1]
    left("core", th)
    left("one", s1)
    left_kind("two", once_only)
    left_kind("last", once_only)
    left_units(sent[None])

    @only("inner")
    def _():
        left_kind("mid", once_only * hops + twice * (2 + hops))
        left_kind("up", once_only + 2 * twice)
        left_pieces(part_sem.at[0], once_only + 2 * twice)
        left_units(sent["inner"])

    @only("outer")
    def _():
        left_kind("low", once_only + 2 * twice)
        left_pieces(part_sem.at[0], once_only)
        left_units(sent["outer"])

    for copy in written:
        copy.wait()


def layer(counts, tokens, gain, key_grad, weight):
    count, features = tokens.shape
    width = key_grad.shape[1]
    rows = weight.shape[0]
    blocks = len(HALVES)
    assert blocks == GROUPS * CUTS
    wide = width // GROUPS
    part = rows // (2 * CUTS)
    hops = 1 + bits_of(counts["rep"]) - 3
    lanes = 128
    stores = blocks + HALVES.count("z")
    any_space = pl.BlockSpec(memory_space=pl.ANY)
    dma = pltpu.SemaphoreType.DMA
    spreads = len(SPREADS)
    scratch = [
        pltpu.VMEM((count, features), BF16),
        pltpu.VMEM((features // lanes, lanes), F32),
        pltpu.VMEM((count, width), BF16),
        pltpu.VMEM((count, features), BF16),
        pltpu.VMEM((features, count), BF16),
        pltpu.VMEM((4, rows, width), BF16),
        pltpu.VMEM((blocks, 2, part, wide), F32),
        pltpu.VMEM((blocks, 2, 2, part, wide), BF16),
        pltpu.VMEM((blocks, 2, 2, part, wide), BF16),
        pltpu.VMEM((blocks, 2, part, wide), BF16),
        pltpu.VMEM((blocks, 2, part, wide), BF16),
        pltpu.VMEM((blocks, part, wide), BF16),
        pltpu.VMEM((blocks, part, wide), BF16),
        pltpu.VMEM((stores, part, wide), BF16),
        pltpu.VMEM((stores, hops, part, wide), BF16),
        pltpu.VMEM((stores, hops, part, wide), BF16),
        pltpu.VMEM((blocks, 2, part, wide), BF16),
        pltpu.VMEM((count, width), F32),
        pltpu.VMEM((count, features), F32),
        pltpu.VMEM((count, features), BF16),
        pltpu.VMEM((count, 1), F32),
        pltpu.VMEM((1, features), F32),
        dma((6,)),
        dma((4,)),
        dma((1,)),
        dma((len(KINDS),)),
        dma((blocks,)),
        dma((blocks, 2)),
        dma((blocks,)),
        dma((stores,)),
        dma((stores, hops)),
        dma((stores,)),
        dma((blocks,)),
        dma((spreads,)),
        dma((spreads, 3)),
        dma((spreads, 2)),
        dma((spreads, 4)),
        dma((1,)),
    ]
    keys, token_grad, grads = pl.pallas_call(
        functools.partial(layer_kernel, counts),
        in_specs=[any_space] * 4,
        out_specs=[any_space] * 3,
        out_shape=[
            jax.ShapeDtypeStruct((count, width), BF16),
            jax.ShapeDtypeStruct((count, features), BF16),
            jax.ShapeDtypeStruct((2 * CUTS, part, width), BF16),
        ],
        scratch_shapes=scratch,
        compiler_params=pltpu.CompilerParams(
            collective_id=0, has_side_effects=True, vmem_limit_bytes=67043328
        ),
        name="layer",
    )(tokens, gain.reshape(features // lanes, lanes), key_grad, weight)
    return keys, token_grad, grads.reshape(rows, width)


def requantize_kernel(
    chunks, sub, grads, m_code, m_exp, v_code, v_exp, keys_in, token_in,
    step, m_rel, m_scale, v_rel, v_scale, keys_out, token_out,
    units, tops, keys, token, sems,
):
    here, last = pl.program_id(0), pl.num_programs(0) - 1
    into = [pltpu.make_async_copy(token_in, token, sems.at[0]), pltpu.make_async_copy(keys_in, keys, sems.at[1])]
    back = [pltpu.make_async_copy(token, token_out, sems.at[2]), pltpu.make_async_copy(keys, keys_out, sems.at[3])]

    @pl.when(here == 0)
    def _():
        for copy in into:
            copy.start()

    rows, width = m_code.shape
    size = width // chunks
    unit_m = jnp.exp2(m_exp[...].astype(F32)) * (0.9 / 127.0)
    unit_v = jnp.exp2(v_exp[...].astype(F32)) * (0.999 / 255.0)
    units[...] = jnp.concatenate([unit_m, unit_v], axis=0).T
    floor = 1e-08 * bias_second**0.5
    rate = bias_second**0.5 / bias_first

    def run(i, carry):
        at = pl.ds(pl.multiple_of(i * sub, sub), sub)
        for c in range(chunks):
            cols = slice(c * size, (c + 1) * size)
            g = grads[at, cols].astype(F32)
            m_new = m_code[at, cols].astype(F32) * units[at, c : c + 1] + 0.1 * g
            v_new = v_code[at, cols].astype(F32) * units[at, chunks + c : chunks + c + 1] + 0.001 * g * g
            root = v_new * lax.rsqrt(v_new)
            step[at, cols] = (m_new * rate) / (root + floor)
            m_top = jnp.max(jnp.abs(m_new), axis=1, keepdims=True)
            v_top = jnp.max(v_new, axis=1, keepdims=True)
            tops[at, c : c + 1] = m_top
            tops[at, chunks + c : chunks + c + 1] = v_top
            m_rel[at, cols] = (m_new * (1.0 / (m_top + 1e-06))).astype(BF16)
            v_rel[at, cols] = (v_new * (1.0 / (v_top + 1e-06))).astype(BF16)
        return carry

    lax.fori_loop(0, rows // sub, run, 0, unroll=True)
    turned = tops[...].T
    m_scale[...] = turned[:chunks]
    v_scale[...] = turned[chunks:]

    @pl.when(here == last - 1)
    def _():
        for one, other in zip(into, back):
            one.wait()
            other.start()

    @pl.when(here == last)
    def _():
        for copy in back:
            copy.wait()


def requantize(grads, m_code, m_exp, v_code, v_exp, keys, token_grad, block=384, sub=128):
    rows, width = m_code.shape
    chunks = m_exp.shape[1]
    wide = pl.BlockSpec((block, width), lambda i: (i, 0))
    thin = pl.BlockSpec((chunks, block), lambda i: (0, i))
    any_space = pl.BlockSpec(memory_space=pl.ANY)
    shape = jax.ShapeDtypeStruct
    step, m_rel, m_scale, v_rel, v_scale, keys, token_grad = pl.pallas_call(
        functools.partial(requantize_kernel, chunks, sub),
        grid=(rows // block,),
        in_specs=[wide, wide, thin, wide, thin, any_space, any_space],
        out_specs=[wide, wide, thin, wide, thin, any_space, any_space],
        out_shape=[
            shape((rows, width), F32),
            shape((rows, width), BF16),
            shape((chunks, rows), F32),
            shape((rows, width), BF16),
            shape((chunks, rows), F32),
            shape(keys.shape, keys.dtype),
            shape(token_grad.shape, token_grad.dtype),
        ],
        scratch_shapes=[
            pltpu.VMEM((block, 2 * chunks), F32),
            pltpu.VMEM((block, 2 * chunks), F32),
            pltpu.VMEM(keys.shape, keys.dtype),
            pltpu.VMEM(token_grad.shape, token_grad.dtype),
            pltpu.SemaphoreType.DMA((4,)),
        ],
        name="requantize",
    )(grads, m_code, m_exp.T, v_code, v_exp.T, keys, token_grad)
    return keys, token_grad, step, m_rel, m_scale.T, v_rel, v_scale.T


def body(counts, tokens, norm_gain, key_grad, key_weight, m_code, m_exp, v_code, v_exp):
    keys, token_grad, grads = layer(counts, tokens, norm_gain, key_grad, key_weight)
    return requantize(grads, m_code, m_exp, v_code, v_exp, keys, token_grad)


def solution(mesh):
    rows = P("shard", None)
    tokens = P(("shard", "rep"), None)
    return jax.shard_map(
        functools.partial(body, dict(mesh.shape)),
        mesh=mesh,
        in_specs=(tokens, P(), tokens, rows, rows, rows, rows, rows),
        out_specs=(tokens, tokens, rows, rows, rows, rows, rows),
        check_vma=False,
    )
```

```python
import functools

import jax
import jax.numpy as jnp
from jax import lax
from jax.experimental import pallas as pl
from jax.experimental.pallas import tpu as pltpu
from jax.sharding import PartitionSpec as P

bias_first = 0.9999734386011124
bias_second = 0.0952078528862904
F32 = jnp.float32
BF16 = jnp.bfloat16

GROUPS = 4
CUTS = 3
HALVES = [
    "x", "x", "y", "z", "y", "x", "y", "y", "y", "y", "y", "y",
]
KINDS = ["core", "one", "two", "low", "mid", "up", "last", "far"]
SPREADS = [2, 4, 2]
ORDER = [
    "N0", "N1", "N2", "GATE", "WX1", "RT", "T.11", "T.7", "T.10", "RO", "WX2", "O.11", "WX0", "O.7", "WF1",
    "T.4", "T.2", "T.0", "T.3", "T.8", "O.4", "C2.11", "C2.7", "O.10", "T.9", "O.0", "WF2", "T.1", "WC", "O.8",
    "T.5", "QA1", "O.2", "QB1", "C3.11", "C3.7", "T.6", "WF0", "C2.0", "C2.8", "C4.7", "O.9", "O.5", "QC1",
    "C4.11", "KO", "C2.10", "C5.7", "KC", "C2.5", "C3.8", "C5.11", "QD1", "BC", "C2.2", "C3.0", "C3.10", "C2.9",
    "C2.4", "O.3", "C3.5", "C4.8", "WG0", "C4.0", "C4.10", "WG2", "O.6", "C3.9", "BO", "C5.0", "C3.2", "C5.8",
    "C4.5", "C4.9", "C5.10", "E5.7", "QE1", "C2.6", "C3.4", "E5.11", "O.1", "KF", "D2.3", "C4.2", "C5.5",
    "E5.0", "KG", "D3.3", "E5.8", "C7.7", "C7.11", "BG", "C7.0", "C2.1", "C5.2", "D4.3", "C3.6", "E5.10",
    "C4.4", "BF", "C4.6", "E5.2", "C3.1", "D5.3", "C7.8", "C5.9", "F0", "C5.4", "F1", "E5.5", "C4.1", "F2",
    "C5.6", "C7.2", "C5.1", "C7.10", "D6.3", "E5.9", "E5.4", "E5.6", "D7.3", "C7.9", "E5.1", "C7.5", "C7.4",
    "C7.6", "D8.3", "C7.1",
]


def bits_of(count):
    bits = count.bit_length() - 1
    assert 1 << bits == count
    return bits


class Labels:
    def __init__(self, counts):
        shards, reps = bits_of(counts["shard"]), bits_of(counts["rep"])
        assert shards == 2 and reps >= 3
        self.me = {axis: lax.axis_index(axis) for axis in ("shard", "rep")}
        self.of = {"c": ("shard", 0), "x": ("shard", 1), "y": ("rep", 0), "l": ("rep", 1)}
        self.extra = [f"h{n}" for n in range(3, reps)]
        for n in range(3, reps):
            self.of[f"h{n}"] = ("rep", n)
        self.bit = {label: self.digit(axis, 1 << n, 2) for label, (axis, n) in self.of.items()}
        self.place = self.digit("rep", 2, 4)
        self.side = lax.div(self.place, jnp.int32(2))
        self.inner = lax.rem(lax.div(self.place + 1, jnp.int32(2)), jnp.int32(2)) == 1

    def digit(self, axis, unit, base):
        return lax.rem(lax.div(self.me[axis], jnp.int32(unit)), jnp.int32(base))

    def device(self, label):
        if label == "m":
            return {"rep": self.me["rep"] + 2 * (3 - 2 * self.place)}
        axis, n = self.of[label]
        return {axis: self.me[axis] + (1 << n) - 2 * (1 << n) * self.bit[label]}


def tiled(rows, step, body):
    def run(i, carry):
        body(pl.ds(pl.multiple_of(i * step, step), step))
        return carry

    lax.fori_loop(0, rows // step, run, 0)


def step_of(rows, most):
    for step in range(most, 0, -1):
        if rows % step == 0 and step % 16 == 0:
            return step
    return rows


def layer_kernel(counts, tokens, gain, key_grad, weight, keys, token_grad, grads, *scratch):
    (x, gains, kg, normed, turned, full, own, th, kc, s1, r1, s2, r2, zr, hs, hr, got, kacc, dn, tg, invs, flat,
     load_sem, out_sem, part_sem, send_sem, core_sem, one_sem, two_sem, low_sem, mid_sem, up_sem, a_sem, wx_sem, wl_sem, wm_sem, wc_sem,
     wo_sem) = scratch
    lab = Labels(counts)
    bit = lab.bit
    tokens_here, features = x.shape
    blocks, _, part, wide = own.shape
    rows = full.shape[1]
    width = kg.shape[1]
    shard = lab.me["shard"]
    core = bit["c"]
    unit = rows // 8
    inner = lab.inner

    def local(src, dst, sem):
        return pltpu.make_async_copy(src, dst, sem)

    def remote(src, dst, came, label, kind):
        return pltpu.make_async_remote_copy(
            src_ref=src, dst_ref=dst, send_sem=send_sem.at[KINDS.index(kind)], recv_sem=came,
            device_id=lab.device(label), device_id_type=pl.DeviceIdType.MESH,
        )

    sent = {None: 0, "inner": 0, "outer": 0}

    def send(copy, role=None, units=0):
        copy.start()
        sent[role] += units

    loaded = []

    def once(load):
        if all(load is not other for other in loaded):
            loaded.append(load)
            load.wait()

    def only(role):
        return pl.when(inner if role == "inner" else jnp.logical_not(inner))

    third = tokens_here // 3
    sixth = tokens_here // 6
    loads = [local(tokens.at[pl.ds(n * sixth, sixth)], x.at[pl.ds(n * sixth, sixth)], load_sem.at[n]) for n in range(6)]
    load_gain = local(gain, gains, load_sem.at[6])
    load_kg = local(key_grad, kg, load_sem.at[7])
    load_w = local(weight, full.at[shard], load_sem.at[8])
    load_gain.start()
    for load in loads:
        load.start()
    load_kg.start()
    load_w.start()

    barrier = pltpu.get_barrier_semaphore()
    greeted = [*lab.of, "m"]
    for label in greeted:
        pl.semaphore_signal(barrier, inc=1, device_id=lab.device(label), device_id_type=pl.DeviceIdType.MESH)
    far = shard + 2 - 4 * bit["x"]
    near = shard + 1 - 2 * core
    both = far + 1 - 2 * core

    def rows_at(place):
        return (2 * place["x"] + place["c"]) * rows + (2 * place["y"] + place["l"]) * part

    tasks = {}

    arrived = []

    def weight_task(n, first, count):
        def at(place):
            return pl.ds(pl.multiple_of((first + place) * unit, 16), unit)

        def move(place, sems, label, shard_at=far):
            ref = full.at[shard_at, at(place)]
            return remote(ref, ref, sems, label, "far")

        place = bit["l"] if count == 2 else lab.place
        beside = place + 1 - 2 * bit["l"]
        across, beyond = 3 - place, 3 - beside
        start = remote(weight.at[at(place)], full.at[shard, at(place)], wx_sem.at[n], "x", "far")
        low = move(place, wl_sem.at[n, 0], "l")
        core0 = move(place, wc_sem.at[n, 0], "c")
        core1 = move(beside, wc_sem.at[n, 1], "c")
        arrived.extend([core0, core1])

        def wx():
            send(start, None, 1)

        tasks[f"WX{n}"] = wx
        if count == 2:
            def wf():
                start.wait_recv()
                send(low, None, 1)
                send(core0, None, 1)

            def wg():
                low.wait_recv()
                send(core1, None, 1)

            tasks[f"WF{n}"], tasks[f"WG{n}"] = wf, wg
            return

        mid0, mid1 = move(place, wm_sem.at[n, 0], "m"), move(beside, wm_sem.at[n, 1], "m")
        up1, up2 = move(across, wl_sem.at[n, 1], "l"), move(beyond, wl_sem.at[n, 2], "l")
        core_a, core_b = move(across, wc_sem.at[n, 2], "c"), move(beyond, wc_sem.at[n, 3], "c")
        end_a, end_b = move(beyond, wc_sem.at[n, 2], "c"), move(across, wc_sem.at[n, 3], "c")
        arrived.extend([core_a, core_b])

        def wf():
            start.wait_recv()
            send(low, None, 1)

            @only("inner")
            def _():
                send(mid0, "inner", 1)

            send(core0, None, 1)

        def qa():
            low.wait_recv()

            @only("inner")
            def _():
                send(mid1, "inner", 1)

            send(core1, None, 1)

        def qb():
            @only("inner")
            def _():
                mid0.wait_recv()
                send(up1, "inner", 1)
                send(core_a, "inner", 1)

        def qc():
            @only("inner")
            def _():
                mid1.wait_recv()
                send(up2, "inner", 1)
                send(core_b, "inner", 1)

        def qd():
            @only("outer")
            def _():
                up1.wait_recv()
                send(end_a, "outer", 1)

        def qe():
            @only("outer")
            def _():
                up2.wait_recv()
                send(end_b, "outer", 1)

        for name, task in dict(WF=wf, QA=qa, QB=qb, QC=qc, QD=qd, QE=qe).items():
            tasks[f"{name}{n}"] = task

    first = 0
    for n, count in enumerate(SPREADS):
        weight_task(n, first, count)
        first += count
    assert first == 8
    own_copy = remote(full.at[shard], full.at[shard], wo_sem.at[0], "c", "far")

    def weight_core():
        once(load_w)
        send(own_copy, None, 8)

    tasks["WC"] = weight_core

    def gate():
        pl.semaphore_wait(barrier, len(greeted))

    tasks["GATE"] = gate

    def norm_task(n):
        def norm():
            if n == 0:
                load_gain.wait()
                flat[...] = jnp.concatenate([gains[k : k + 1, :] for k in range(features // gains.shape[1])], axis=1)
            for half in range(2):
                loads[2 * n + half].wait()
                if n:
                    turn(1 - core, n - 1, half)
                for i in range(sixth // 16):
                    at = pl.ds(n * third + half * sixth + i * 16, 16)
                    value = x[at, :].astype(F32)
                    inv = lax.rsqrt(jnp.mean(value * value, axis=1, keepdims=True) + 1e-06)
                    invs[at, :] = inv
                    normed[at, :] = (value * inv * flat[...]).astype(BF16)

        tasks[f"N{n}"] = norm

    def turn(half, n, a):
        here = slice(n * third, (n + 1) * third)
        for i in range(rows // 128):
            at = pl.ds(pl.multiple_of((2 * a + half) * rows + i * 128, 128), 128)
            turned[at, here] = normed[here, at].T

    def turn_task(name, half):
        def task():
            if half is core:
                for a in range(2):
                    base = (2 * a + half) * rows

                    def run(i, carry):
                        at = pl.ds(pl.multiple_of(base + i * 128, 128), 128)
                        turned[at, :] = normed[:, at].T
                        return carry

                    lax.fori_loop(0, rows // 128, run, 0, unroll=3)
            else:
                for a in range(2):
                    turn(half, 2, a)

        tasks[name] = task

    for n in range(3):
        norm_task(n)

    turn_task("RT", 1 - core)
    turn_task("RO", core)
    for n in range(3):
        norm_task(n)

    def outer(place, b):
        g, k = b // CUTS, b % CUTS
        start = (2 * place["x"] + place["c"]) * rows + (CUTS * place["y"] + k) * part
        at = pl.ds(pl.multiple_of(start, 16), part)
        return jnp.dot(turned[at, :], kg[:, g * wide : (g + 1) * wide], preferred_element_type=F32)

    step = step_of(part, 96)

    def late_tasks(b, one, out_at, finish_part):
        e = blocks + HALVES[:b].count("z")
        second = lab.side
        spots = (1 - second, second)
        stores = (b, e)
        lanes = ["y", *lab.extra]
        lows = [remote(hs.at[s, 0], zr.at[s], low_sem.at[s], "l", "low") for s in stores]
        over = remote(hs.at[b, 0], hr.at[b, 0], mid_sem.at[b, 0], "m", "mid")
        chain = [remote(hs.at[e, n], hr.at[e, n], mid_sem.at[e, n], label, "mid") for n, label in enumerate(lanes)]
        mine, other = got.at[b], got.at[e]
        back = remote(mine, other, a_sem.at[b], "m", "mid")
        ups = [remote(mine, out_at(second), up_sem.at[b], "l", "up"), remote(other, out_at(1 - second), up_sem.at[e], "l", "up")]

        def total(n, at):
            return own[b, spots[n], at, :] + r1[b, spots[n], at, :].astype(F32)

        def down(n):
            @only("outer")
            def _():
                one[n].wait_recv()

                def add(at):
                    hs[stores[n], 0, at, :] = total(n, at).astype(BF16)

                tiled(part, step, add)
                send(lows[n], "outer")

        def fourth():
            @only("inner")
            def _():
                one[0].wait_recv()
                lows[0].wait_recv()

                def add(at):
                    hs[b, 0, at, :] = (total(0, at) + zr[b, at, :].astype(F32)).astype(BF16)

                tiled(part, step, add)
                send(over, "inner")

        def fifth():
            @only("inner")
            def _():
                one[1].wait_recv()
                lows[1].wait_recv()
                over.wait_recv()

                def add(at):
                    value = total(1, at) + zr[e, at, :].astype(F32)
                    hs[e, 0, at, :] = (value + hr[b, 0, at, :].astype(F32)).astype(BF16)

                tiled(part, step, add)
                send(chain[0], "inner")

        def sixth():
            @only("inner")
            def _():
                for n in range(len(chain)):
                    chain[n].wait_recv()

                    def add(at):
                        value = (hs[e, n, at, :].astype(F32) + hr[e, n, at, :].astype(F32)).astype(BF16)
                        if n + 1 == len(chain):
                            got[b, at, :] = value
                        else:
                            hs[e, n + 1, at, :] = value

                    tiled(part, step, add)
                    if n + 1 < len(chain):
                        send(chain[n + 1], "inner")
                send(back, "inner")
                send(ups[0], "inner")
                finish_part(second)

        def seventh():
            @only("inner")
            def _():
                back.wait_recv()
                send(ups[1], "inner")
                finish_part(1 - second, e)

        def eighth():
            @only("outer")
            def _():
                for copy in ups:
                    copy.wait_recv()

        return dict(D2=lambda: down(0), D3=lambda: down(1), D4=fourth, D5=fifth, D6=sixth, D7=seventh, D8=eighth)

    def block_tasks(b):
        late = HALVES[b] == "z"
        o1 = "y" if HALVES[b] == "y" else "x"
        o2 = "x" if o1 == "y" else "y"
        b1 = bit[o1]
        b2 = lab.side if late else bit[o2]
        g, k = b // CUTS, b % CUTS
        def out_at(y):
            return grads.at[CUTS * y + k, :, pl.ds(g * wide, wide)]

        over = remote(th.at[b], kc.at[b], core_sem.at[b], "c", "core")
        one = [remote(s1.at[b, j], r1.at[b, j], one_sem.at[b, n], o1, "one") for n, j in enumerate((1 - b2, b2))]
        two = remote(s2.at[b], r2.at[b], two_sem.at[b], o2, "two")
        low = remote(hs.at[b, 0], zr.at[b], low_sem.at[b], "l", "low")
        lanes = ["m", *lab.extra]
        mids = [remote(hs.at[b, n], hr.at[b, n], mid_sem.at[b, n], label, "mid") for n, label in enumerate(lanes)]
        mine = got.at[b]
        up = remote(mine, mine, up_sem.at[b], "l", "up")
        last = remote(mine, out_at(bit["y"]), a_sem.at[b], "y", "last")

        def theirs():
            once(load_kg)
            for a in range(2):
                for y in range(2):
                    th[b, a, y] = outer({"x": a, "y": y, "c": 1 - core}, b).astype(BF16)
            send(over)

        def ours():
            over.wait_recv()

            def piece(first, second):
                place = {o1: first, o2: second, "c": core}
                return outer(place, b) + kc[b, place["x"], place["y"]].astype(F32)

            for n, j in enumerate((1 - b2, b2)):
                s1[b, j] = piece(1 - b1, j).astype(BF16)
                send(one[n])
            for j in range(2):
                own[b, j] = piece(b1, j)

        def second():
            one[0].wait_recv()

            def add(at):
                s2[b, at, :] = (own[b, 1 - b2, at, :] + r1[b, 1 - b2, at, :].astype(F32)).astype(BF16)

            tiled(part, step, add)
            send(two)

        def total(at):
            value = own[b, b2, at, :] + r1[b, b2, at, :].astype(F32)
            return value + r2[b, at, :].astype(F32)

        def third_step():
            @only("outer")
            def _():
                one[1].wait_recv()
                two.wait_recv()

                def add(at):
                    hs[b, 0, at, :] = total(at).astype(BF16)

                tiled(part, step, add)
                send(low, "outer")

        def fourth():
            @only("inner")
            def _():
                one[1].wait_recv()
                two.wait_recv()
                low.wait_recv()

                def add(at):
                    hs[b, 0, at, :] = (total(at) + zr[b, at, :].astype(F32)).astype(BF16)

                tiled(part, step, add)
                send(mids[0], "inner")

        def fifth():
            @only("inner")
            def _():
                for n in range(len(mids)):
                    mids[n].wait_recv()

                    def add(at):
                        value = (hs[b, n, at, :].astype(F32) + hr[b, n, at, :].astype(F32)).astype(BF16)
                        if n + 1 == len(mids):
                            got[b, at, :] = value
                        else:
                            hs[b, n + 1, at, :] = value

                    tiled(part, step, add)
                    if n + 1 < len(mids):
                        send(mids[n + 1], "inner")
                send(up, "inner")
                send(last, "inner")

        def ends():
            @only("outer")
            def _():
                up.wait_recv()
                send(last, "outer")

            finish_part(bit["y"])

        def finish_part(y, spot=b):
            local(got.at[spot], out_at(y), part_sem.at[0]).start()

        def seventh():
            last.wait_recv()

        if late:
            names = dict(T=theirs, O=ours, **late_tasks(b, one, out_at, finish_part))
        else:
            names = dict(T=theirs, O=ours, C2=second, C3=third_step, C4=fourth, C5=fifth, E5=ends, C7=seventh)
        for name, task in names.items():
            tasks[f"{name}.{b}"] = task

    written = []

    def put(copy):
        copy.start()
        written.append(copy)

    for b in range(blocks):
        block_tasks(b)

    def forward(index, first):
        base = pl.multiple_of(index * rows, 128)

        def key_part(t, carry):
            at = pl.ds(pl.multiple_of(t * 256, 256), 256)
            total = jnp.dot(normed[:, pl.ds(base, rows)], full[index, :, at], preferred_element_type=F32)
            if first:
                kacc[:, at] = total
            else:
                kacc[:, at] += total
            return carry

        lax.fori_loop(0, width // 256, key_part, 0, unroll=2)

    def backward(index):
        base = pl.multiple_of(index * rows, 128)
        cut = 384

        def back_part(t, carry):
            at = pl.ds(pl.multiple_of(t * cut, 128), cut)
            to = pl.ds(pl.multiple_of(base + t * cut, 128), cut)
            dn[:, to] = lax.dot_general(
                kg[...], full[index, at, :], (((1,), (1,)), ((), ())), preferred_element_type=F32
            )
            return carry

        lax.fori_loop(0, rows // cut, back_part, 0)

    def own_forward():
        once(load_w)
        forward(shard, True)

    def own_backward():
        once(load_w)
        once(load_kg)
        backward(shard)

    def near_forward():
        own_copy.wait_recv()
        forward(near, False)

    def both_forward():
        for copy in arrived:
            copy.wait_recv()
        forward(both, False)

    tasks.update(
        KO=own_forward, BO=own_backward,
        KC=near_forward, BC=lambda: backward(near),
        KF=lambda: forward(far, False), BF=lambda: backward(far),
        KG=both_forward, BG=lambda: backward(both),
    )

    def finish_task(n):
        def finish():
            def run(i, carry):
                at = pl.ds(pl.multiple_of(n * third + i * 16, 16), 16)
                value = x[at, :].astype(F32)
                inv = invs[at, :]
                scaled = dn[at, :] * flat[...]
                inner = jnp.mean(scaled * value, axis=1, keepdims=True)
                tg[at, :] = (inv * scaled - value * (inv * inv * inv * inner)).astype(BF16)
                return carry

            lax.fori_loop(0, third // 16, run, 0, unroll=2)
            at = pl.ds(n * third, third)
            put(local(tg.at[at], token_grad.at[at], out_sem.at[n]))
            if n == 2:
                assert all(ORDER.index(f"O.{b}") < ORDER.index("F2") for b in range(blocks))
                kg[...] = kacc[...].astype(BF16)
                put(local(kg, keys, out_sem.at[3]))

        tasks[f"F{n}"] = finish

    for n in range(3):
        finish_task(n)

    assert sorted(ORDER) == sorted(tasks)
    for name in ORDER:
        tasks[name]()

    def left(kind, ref):
        local(ref, ref, send_sem.at[KINDS.index(kind)]).wait()

    def left_units(count):
        if count >= 8:
            left("far", full.at[pl.ds(0, count // 8)])
        if count % 8:
            left("far", full.at[0, pl.ds(0, count % 8 * unit)])

    def left_pieces(sem, count):
        while count > 0:
            take = min(count, 2 * blocks)
            for ref in ([s1.at[pl.ds(0, take // 2)]] if take > 1 else []) + ([s1.at[0, 0]] if take % 2 else []):
                local(ref, ref, sem).wait()
            count -= take

    def left_kind(kind, count):
        left_pieces(send_sem.at[KINDS.index(kind)], count)

    twice = HALVES.count("z")
    once_only = blocks - twice
    hops = hs.shape[1]
    left("core", th)
    left("one", s1)
    left_kind("two", once_only)
    left_kind("last", once_only)
    left_units(sent[None])

    @only("inner")
    def _():
        left_kind("mid", once_only * hops + twice * (2 + hops))
        left_kind("up", once_only + 2 * twice)
        left_pieces(part_sem.at[0], once_only + 2 * twice)
        left_units(sent["inner"])

    @only("outer")
    def _():
        left_kind("low", once_only + 2 * twice)
        left_pieces(part_sem.at[0], once_only)
        left_units(sent["outer"])

    for copy in written:
        copy.wait()


def layer(counts, tokens, gain, key_grad, weight):
    count, features = tokens.shape
    width = key_grad.shape[1]
    rows = weight.shape[0]
    blocks = len(HALVES)
    assert blocks == GROUPS * CUTS
    wide = width // GROUPS
    part = rows // (2 * CUTS)
    hops = 1 + bits_of(counts["rep"]) - 3
    lanes = 128
    stores = blocks + HALVES.count("z")
    any_space = pl.BlockSpec(memory_space=pl.ANY)
    dma = pltpu.SemaphoreType.DMA
    spreads = len(SPREADS)
    scratch = [
        pltpu.VMEM((count, features), BF16),
        pltpu.VMEM((features // lanes, lanes), F32),
        pltpu.VMEM((count, width), BF16),
        pltpu.VMEM((count, features), BF16),
        pltpu.VMEM((features, count), BF16),
        pltpu.VMEM((4, rows, width), BF16),
        pltpu.VMEM((blocks, 2, part, wide), F32),
        pltpu.VMEM((blocks, 2, 2, part, wide), BF16),
        pltpu.VMEM((blocks, 2, 2, part, wide), BF16),
        pltpu.VMEM((blocks, 2, part, wide), BF16),
        pltpu.VMEM((blocks, 2, part, wide), BF16),
        pltpu.VMEM((blocks, part, wide), BF16),
        pltpu.VMEM((blocks, part, wide), BF16),
        pltpu.VMEM((stores, part, wide), BF16),
        pltpu.VMEM((stores, hops, part, wide), BF16),
        pltpu.VMEM((stores, hops, part, wide), BF16),
        pltpu.VMEM((stores, part, wide), BF16),
        pltpu.VMEM((count, width), F32),
        pltpu.VMEM((count, features), F32),
        pltpu.VMEM((count, features), BF16),
        pltpu.VMEM((count, 1), F32),
        pltpu.VMEM((1, features), F32),
        dma((9,)),
        dma((4,)),
        dma((1,)),
        dma((len(KINDS),)),
        dma((blocks,)),
        dma((blocks, 2)),
        dma((blocks,)),
        dma((stores,)),
        dma((stores, hops)),
        dma((stores,)),
        dma((blocks,)),
        dma((spreads,)),
        dma((spreads, 3)),
        dma((spreads, 2)),
        dma((spreads, 4)),
        dma((1,)),
    ]
    keys, token_grad, grads = pl.pallas_call(
        functools.partial(layer_kernel, counts),
        in_specs=[any_space] * 4,
        out_specs=[any_space] * 3,
        out_shape=[
            jax.ShapeDtypeStruct((count, width), BF16),
            jax.ShapeDtypeStruct((count, features), BF16),
            jax.ShapeDtypeStruct((2 * CUTS, part, width), BF16),
        ],
        scratch_shapes=scratch,
        compiler_params=pltpu.CompilerParams(
            collective_id=0, has_side_effects=True, vmem_limit_bytes=67043328
        ),
        name="layer",
    )(tokens, gain.reshape(features // lanes, lanes), key_grad, weight)
    return keys, token_grad, grads.reshape(rows, width)


def requantize_kernel(chunks, block, ahead, *refs):
    ins, outs = refs[:5], refs[7:12]
    pass_in, pass_out = refs[5:7], refs[12:14]
    grads, m_code, v_code, m_exp, v_exp, step, m_rel, v_rel, m_scale, v_scale, units = refs[14:25]
    passed = refs[25:27]
    in_sem, exp_sem, out_sem, scale_sem, pass_sem = refs[27:]
    rows, width = m_code.shape
    size = width // chunks
    count = rows // block

    def at_block(i):
        return pl.ds(pl.multiple_of(i * block, block), block)

    def load(i, n):
        return pltpu.make_async_copy(ins[n].at[at_block(i)], (grads, m_code, v_code)[n].at[at_block(i)], in_sem.at[i, n])

    def store(i, n):
        return pltpu.make_async_copy((step, m_rel, v_rel)[n].at[at_block(i)], outs[n].at[at_block(i)], out_sem.at[i, n])

    exps = [pltpu.make_async_copy(ins[3 + n], (m_exp, v_exp)[n], exp_sem.at[n]) for n in range(2)]
    scales = [pltpu.make_async_copy((m_scale, v_scale)[n], outs[3 + n], scale_sem.at[n]) for n in range(2)]
    into = [pltpu.make_async_copy(pass_in[n], passed[n], pass_sem.at[n]) for n in range(2)]
    back = [pltpu.make_async_copy(passed[n], pass_out[n], pass_sem.at[2 + n]) for n in range(2)]

    for copy in exps:
        copy.start()
    for i in range(ahead):
        for n in range(3):
            load(i, n).start()
    for copy in into:
        copy.start()
    for copy in exps:
        copy.wait()
    unit_m = jnp.exp2(m_exp[...].astype(F32)) * (0.9 / 127.0)
    unit_v = jnp.exp2(v_exp[...].astype(F32)) * (0.999 / 255.0)
    units[...] = jnp.concatenate([unit_m, unit_v], axis=0).T
    floor = 1e-08 * bias_second**0.5
    rate = bias_second**0.5 / bias_first

    def run(i, carry):
        @pl.when(i + ahead < count)
        def _():
            for n in range(3):
                load(i + ahead, n).start()

        for n in range(3):
            load(i, n).wait()
        at = at_block(i)
        tops = [], []
        for c in range(chunks):
            cols = slice(c * size, (c + 1) * size)
            g = grads[at, cols].astype(F32)
            m_new = m_code[at, cols].astype(F32) * units[at, c : c + 1] + 0.1 * g
            v_new = v_code[at, cols].astype(F32) * units[at, chunks + c : chunks + c + 1] + 0.001 * g * g
            root = v_new * lax.rsqrt(v_new)
            step[at, cols] = (m_new * rate) / (root + floor)
            m_top = jnp.max(jnp.abs(m_new), axis=1, keepdims=True)
            v_top = jnp.max(v_new, axis=1, keepdims=True)
            tops[0].append(m_top)
            tops[1].append(v_top)
            m_rel[at, cols] = (m_new * (1.0 / (m_top + 1e-06))).astype(BF16)
            v_rel[at, cols] = (v_new * (1.0 / (v_top + 1e-06))).astype(BF16)
        turned = jnp.concatenate(tops[0] + tops[1], axis=1).T
        m_scale[:, at] = turned[:chunks]
        v_scale[:, at] = turned[chunks:]
        for n in range(3):
            store(i, n).start()

        @pl.when(i == count // 2)
        def _():
            for one, other in zip(into, back):
                one.wait()
                other.start()

        return carry

    lax.fori_loop(0, count, run, 0)
    for copy in scales:
        copy.start()

    def drain(i, carry):
        for n in range(3):
            store(i, n).wait()
        return carry

    lax.fori_loop(0, count, drain, 0)
    for copy in back + scales:
        copy.wait()


def requantize(grads, m_code, m_exp, v_code, v_exp, keys, token_grad, block=128, ahead=4):
    rows, width = m_code.shape
    chunks = m_exp.shape[1]
    count = rows // block
    any_space = pl.BlockSpec(memory_space=pl.ANY)
    shape = jax.ShapeDtypeStruct
    dma = pltpu.SemaphoreType.DMA
    step, m_rel, v_rel, m_scale, v_scale, keys, token_grad = pl.pallas_call(
        functools.partial(requantize_kernel, chunks, block, min(ahead, count)),
        in_specs=[any_space] * 7,
        out_specs=[any_space] * 7,
        out_shape=[
            shape((rows, width), F32),
            shape((rows, width), BF16),
            shape((rows, width), BF16),
            shape((chunks, rows), F32),
            shape((chunks, rows), F32),
            shape(keys.shape, keys.dtype),
            shape(token_grad.shape, token_grad.dtype),
        ],
        scratch_shapes=[
            pltpu.VMEM((rows, width), BF16),
            pltpu.VMEM((rows, width), BF16),
            pltpu.VMEM((rows, width), BF16),
            pltpu.VMEM((chunks, rows), jnp.int32),
            pltpu.VMEM((chunks, rows), jnp.int32),
            pltpu.VMEM((rows, width), F32),
            pltpu.VMEM((rows, width), BF16),
            pltpu.VMEM((rows, width), BF16),
            pltpu.VMEM((chunks, rows), F32),
            pltpu.VMEM((chunks, rows), F32),
            pltpu.VMEM((rows, 2 * chunks), F32),
            pltpu.VMEM(keys.shape, keys.dtype),
            pltpu.VMEM(token_grad.shape, token_grad.dtype),
            dma((count, 3)),
            dma((2,)),
            dma((count, 3)),
            dma((2,)),
            dma((4,)),
        ],
        name="requantize",
    )(grads, m_code, v_code, m_exp.T, v_exp.T, keys, token_grad)
    return keys, token_grad, step, m_rel, m_scale.T, v_rel, v_scale.T


def body(counts, tokens, norm_gain, key_grad, key_weight, m_code, m_exp, v_code, v_exp):
    keys, token_grad, grads = layer(counts, tokens, norm_gain, key_grad, key_weight)
    return requantize(grads, m_code, m_exp, v_code, v_exp, keys, token_grad)


def solution(mesh):
    rows = P("shard", None)
    tokens = P(("shard", "rep"), None)
    return jax.shard_map(
        functools.partial(body, dict(mesh.shape)),
        mesh=mesh,
        in_specs=(tokens, P(), tokens, rows, rows, rows, rows, rows),
        out_specs=(tokens, tokens, rows, rows, rows, rows, rows),
        check_vma=False,
    )
```
